8 devices in a mesh: dp: 1 (over z), ep: 8 (over y, x, core).
Axes of the slice: x: 2, y: 2, z: 1, core: 2. Of those that a mesh axis runs over, the one named last changes fastest.
Arguments:
- hidden: bfloat16 [256, 7168], P(('dp', 'ep'))
- positions: int32 [256], P(('dp', 'ep'))
- ckv_cache: bfloat16 [256, 64, 512], P(('dp', 'ep'))
- kpe_cache: bfloat16 [256, 64, 64], P(('dp', 'ep'))
- topk_ids: int32 [256, 8], P(('dp', 'ep'))
- attn_gain: bfloat16 [7168], replicated
- w_dq: bfloat16 [7168, 1536], replicated
- q_gain: bfloat16 [1536], replicated
- w_uq: bfloat16 [1536, 3072], replicated
- w_dkv: bfloat16 [7168, 576], replicated
- kv_gain: bfloat16 [512], replicated
- w_uk: bfloat16 [512, 2048], replicated
- w_uv: bfloat16 [512, 2048], replicated
- w_out: bfloat16 [2048, 7168], replicated
- ffn_gain: bfloat16 [7168], replicated
- w_router: bfloat16 [7168, 16], replicated
- w_gate: bfloat16 [16, 7168, 2048], P('ep')
- w_up: bfloat16 [16, 7168, 2048], P('ep')
- w_down: bfloat16 [16, 2048, 7168], P('ep')
- shared_gate: bfloat16 [7168, 2048], replicated
- shared_up: bfloat16 [7168, 2048], replicated
- shared_down: bfloat16 [2048, 7168], replicated
Outputs:
- output 1: bfloat16 [256, 7168], P(('dp', 'ep'))
- output 2: bfloat16 [256, 512], P(('dp', 'ep'))
- output 3: bfloat16 [256, 64], P(('dp', 'ep'))
All inputs are finite; a program needn't handle non-finite values.
Results may differ from the reference program's by a relative error of at most 0.0153635.
Values are sent between devices in bfloat16 or wider.
A program may use at most 1.5 GiB of HBM per device.

```python
import jax
import jax.numpy as jnp
from jax import lax

MODEL_DIM = 7168
HEADS = 16
Q_RANK = 1536
KV_RANK = 512
NOPE_DIM = 128
ROPE_DIM = 64
VALUE_DIM = 128
EXPERTS = 16
EXPERT_FF = 2048
SHARED_FF = 2048
TOP_K = 8
N_GROUPS = 8
TOP_GROUPS = 4
TOKENS_DEV = 32
EP_SIZE = 8
CACHE_LEN = 64
CAPACITY = 32

BATCH_PART = EP_SIZE * TOKENS_DEV
QK_DIM = NOPE_DIM + ROPE_DIM
EPSILON = 1e-6
ROUTE_SCALE = 2.5
ROPE_BASE = 10000.0


def draw_routing(key):
    keys = jax.random.split(key, 2)
    rank_of = jax.random.permutation(keys[0], EXPERTS)
    popular = jnp.where(rank_of == 0, 1048576, 4096 // (rank_of + 1))
    noise = jax.random.randint(keys[1], (BATCH_PART, EXPERTS), 0, 4096)
    score = (popular[None, :] + noise) * EXPERTS + jnp.arange(EXPERTS)[None, :]
    group_best = jnp.max(score.reshape(BATCH_PART, N_GROUPS, EXPERTS // N_GROUPS), axis=2)
    group_ids = lax.top_k(group_best, TOP_GROUPS)[1]
    chosen = jnp.any(group_ids[:, :, None] == jnp.arange(N_GROUPS)[None, None, :], axis=1)
    allowed = jnp.repeat(chosen, EXPERTS // N_GROUPS, axis=1)
    masked = jnp.where(allowed, score, -1)
    return lax.top_k(masked, TOP_K)[1].astype(jnp.int32)


def draw_positions(key):
    keys = jax.random.split(key, 2)
    limit = jax.random.randint(keys[0], (EP_SIZE, 1), CACHE_LEN // 8, CACHE_LEN + 1)
    positions = jax.random.randint(keys[1], (EP_SIZE, TOKENS_DEV), 0, limit).reshape(BATCH_PART)
    return positions.at[0].set(CACHE_LEN - 1).astype(jnp.int32)


def draw_normal(key, shape, scale):
    return (jax.random.normal(key, shape, jnp.float32) * scale).astype(jnp.bfloat16)


def draw_gain(key, shape):
    return jax.random.uniform(key, shape, jnp.float32, 0.5, 1.5).astype(jnp.bfloat16)


def draw_stack(key, shape, scale):
    return lax.map(lambda one: draw_normal(one, shape, scale), jax.random.split(key, EXPERTS))


def setup_inputs(seed: int = 0, part: int = 0) -> dict:
    wkeys = jax.random.split(jax.random.key(seed + 1), 18)
    pkeys = jax.random.split(jax.random.fold_in(jax.random.key(seed), part), 6)
    ckv_mean = 0.5 * jax.random.normal(pkeys[2], (BATCH_PART, 1, KV_RANK), jnp.float32)
    ckv_rows = jax.random.normal(pkeys[3], (BATCH_PART, CACHE_LEN, KV_RANK), jnp.float32)
    return {
        'hidden': draw_normal(pkeys[0], (BATCH_PART, MODEL_DIM), 1.0),
        'positions': draw_positions(pkeys[1]),
        'ckv_cache': (ckv_mean + ckv_rows).astype(jnp.bfloat16),
        'kpe_cache': draw_normal(pkeys[4], (BATCH_PART, CACHE_LEN, ROPE_DIM), 1.0),
        'topk_ids': draw_routing(pkeys[5]),
        'attn_gain': draw_gain(wkeys[0], (MODEL_DIM,)),
        'w_dq': draw_normal(wkeys[1], (MODEL_DIM, Q_RANK), MODEL_DIM ** -0.5),
        'q_gain': draw_gain(wkeys[2], (Q_RANK,)),
        'w_uq': draw_normal(wkeys[3], (Q_RANK, HEADS * QK_DIM), Q_RANK ** -0.5),
        'w_dkv': draw_normal(wkeys[4], (MODEL_DIM, KV_RANK + ROPE_DIM), MODEL_DIM ** -0.5),
        'kv_gain': draw_gain(wkeys[5], (KV_RANK,)),
        'w_uk': draw_normal(wkeys[6], (KV_RANK, HEADS * NOPE_DIM), KV_RANK ** -0.5),
        'w_uv': draw_normal(wkeys[7], (KV_RANK, HEADS * VALUE_DIM), KV_RANK ** -0.5),
        'w_out': draw_normal(wkeys[8], (HEADS * VALUE_DIM, MODEL_DIM), (HEADS * VALUE_DIM) ** -0.5),
        'ffn_gain': draw_gain(wkeys[9], (MODEL_DIM,)),
        'w_router': draw_normal(wkeys[10], (MODEL_DIM, EXPERTS), 1.2 * MODEL_DIM ** -0.5),
        'w_gate': draw_stack(wkeys[11], (MODEL_DIM, EXPERT_FF), MODEL_DIM ** -0.5),
        'w_up': draw_stack(wkeys[12], (MODEL_DIM, EXPERT_FF), MODEL_DIM ** -0.5),
        'w_down': draw_stack(wkeys[13], (EXPERT_FF, MODEL_DIM), 2.0 * EXPERT_FF ** -0.5),
        'shared_gate': draw_normal(wkeys[14], (MODEL_DIM, SHARED_FF), MODEL_DIM ** -0.5),
        'shared_up': draw_normal(wkeys[15], (MODEL_DIM, SHARED_FF), MODEL_DIM ** -0.5),
        'shared_down': draw_normal(wkeys[16], (SHARED_FF, MODEL_DIM), 2.0 * SHARED_FF ** -0.5),
    }


def rms_norm(vec, gain):
    vec = vec.astype(jnp.float32)
    scale = lax.rsqrt(jnp.mean(vec * vec, axis=-1, keepdims=True) + EPSILON)
    return vec * scale * gain.astype(jnp.float32)


def rotary(vec, positions):
    half = ROPE_DIM // 2
    freqs = ROPE_BASE ** (-jnp.arange(half).astype(jnp.float32) / half)
    angle = positions.astype(jnp.float32)[..., None] * freqs
    cosine = jnp.cos(angle)
    sine = jnp.sin(angle)
    first = vec[..., :half]
    second = vec[..., half:]
    return jnp.concatenate([first * cosine - second * sine, first * sine + second * cosine], axis=-1)


def attend_one(args):
    q_abs, q_rot, ckv_rows, kpe_rows, c_new, k_new, position = args
    scale = QK_DIM ** -0.5
    s_cache = (jnp.dot(q_abs, ckv_rows.T, preferred_element_type=jnp.float32) + jnp.dot(q_rot, kpe_rows.T, preferred_element_type=jnp.float32)) * scale
    valid = jnp.arange(CACHE_LEN) < position
    s_cache = jnp.where(valid[None, :], s_cache, -1e30)
    s_self = (jnp.dot(q_abs, c_new, preferred_element_type=jnp.float32) + jnp.dot(q_rot, k_new, preferred_element_type=jnp.float32)) * scale
    peak = jnp.maximum(jnp.max(s_cache, axis=1), s_self)
    e_cache = jnp.exp(s_cache - peak[:, None])
    e_self = jnp.exp(s_self - peak)
    denominator = jnp.sum(e_cache, axis=1) + e_self
    p_cache = (e_cache / denominator[:, None]).astype(jnp.bfloat16)
    p_self = (e_self / denominator).astype(jnp.bfloat16)
    context = jnp.dot(p_cache, ckv_rows, preferred_element_type=jnp.float32) + p_self.astype(jnp.float32)[:, None] * c_new.astype(jnp.float32)[None, :]
    return context.astype(jnp.bfloat16)


def expert_apply(args):
    rows, gate_w, up_w, down_w = args
    h_gate = jnp.dot(rows, gate_w, preferred_element_type=jnp.float32)
    h_up = jnp.dot(rows, up_w, preferred_element_type=jnp.float32)
    act = (jax.nn.silu(h_gate) * h_up).astype(jnp.bfloat16)
    return jnp.dot(act, down_w, preferred_element_type=jnp.float32).astype(jnp.bfloat16)


def reference(hidden, positions, ckv_cache, kpe_cache, topk_ids, attn_gain, w_dq, q_gain, w_uq, w_dkv, kv_gain, w_uk, w_uv, w_out, ffn_gain, w_router, w_gate, w_up, w_down, shared_gate, shared_up, shared_down):
    normed = rms_norm(hidden, attn_gain).astype(jnp.bfloat16)
    c_q = rms_norm(jnp.dot(normed, w_dq, preferred_element_type=jnp.float32), q_gain).astype(jnp.bfloat16)
    query = jnp.dot(c_q, w_uq, preferred_element_type=jnp.float32).astype(jnp.bfloat16).reshape(BATCH_PART, HEADS, QK_DIM)
    q_nope = query[:, :, :NOPE_DIM]
    q_rot = rotary(query[:, :, NOPE_DIM:].astype(jnp.float32), positions[:, None]).astype(jnp.bfloat16)
    kv_proj = jnp.dot(normed, w_dkv, preferred_element_type=jnp.float32)
    c_new = rms_norm(kv_proj[:, :KV_RANK], kv_gain).astype(jnp.bfloat16)
    k_new = rotary(kv_proj[:, KV_RANK:], positions).astype(jnp.bfloat16)
    q_abs = jnp.einsum('bhn,chn->bhc', q_nope.astype(jnp.float32), w_uk.reshape(KV_RANK, HEADS, NOPE_DIM).astype(jnp.float32)).astype(jnp.bfloat16)
    context = lax.map(attend_one, (q_abs, q_rot, ckv_cache, kpe_cache, c_new, k_new, positions))
    heads_out = jnp.einsum('bhc,chv->bhv', context.astype(jnp.float32), w_uv.reshape(KV_RANK, HEADS, VALUE_DIM).astype(jnp.float32)).astype(jnp.bfloat16)
    attn_out = jnp.dot(heads_out.reshape(BATCH_PART, HEADS * VALUE_DIM), w_out, preferred_element_type=jnp.float32)
    x_mid = (hidden.astype(jnp.float32) + attn_out).astype(jnp.bfloat16)
    u_norm = rms_norm(x_mid, ffn_gain).astype(jnp.bfloat16)
    gates = jax.nn.sigmoid(jnp.dot(u_norm, w_router, preferred_element_type=jnp.float32))
    chosen = jnp.take_along_axis(gates, topk_ids, axis=1)
    weights = ROUTE_SCALE * chosen / jnp.sum(chosen, axis=1, keepdims=True)
    hits = (topk_ids[:, :, None] == jnp.arange(EXPERTS)[None, None, :]).astype(jnp.int32)
    per_token = jnp.sum(hits, axis=1).reshape(EP_SIZE, TOKENS_DEV, EXPERTS)
    before = (jnp.cumsum(per_token, axis=1) - per_token).reshape(BATCH_PART, EXPERTS)
    rank = jnp.sum(hits * before[:, None, :], axis=2)
    keep = rank < CAPACITY
    source = jnp.arange(BATCH_PART) // TOKENS_DEV
    target_row = jnp.where(keep, topk_ids * (EP_SIZE * CAPACITY) + source[:, None] * CAPACITY + rank, EXPERTS * EP_SIZE * CAPACITY)
    rows_all = jnp.broadcast_to(u_norm[:, None, :], (BATCH_PART, TOP_K, MODEL_DIM)).reshape(BATCH_PART * TOP_K, MODEL_DIM)
    buffer = jnp.zeros((EXPERTS * EP_SIZE * CAPACITY + 1, MODEL_DIM), jnp.bfloat16).at[target_row.reshape(-1)].set(rows_all)
    buffer = buffer[:-1].reshape(EXPERTS, EP_SIZE * CAPACITY, MODEL_DIM)
    results = lax.map(expert_apply, (buffer, w_gate, w_up, w_down)).reshape(EXPERTS * EP_SIZE * CAPACITY, MODEL_DIM)
    results = jnp.concatenate([results, jnp.zeros((1, MODEL_DIM), jnp.bfloat16)], axis=0)
    picked = jnp.take(results, target_row, axis=0).astype(jnp.float32)
    routed = jnp.sum(weights[:, :, None] * picked, axis=1)
    shared_act = (jax.nn.silu(jnp.dot(u_norm, shared_gate, preferred_element_type=jnp.float32)) * jnp.dot(u_norm, shared_up, preferred_element_type=jnp.float32)).astype(jnp.bfloat16)
    shared_out = jnp.dot(shared_act, shared_down, preferred_element_type=jnp.float32).astype(jnp.bfloat16)
    hidden_out = (x_mid.astype(jnp.float32) + routed + shared_out.astype(jnp.float32)).astype(jnp.bfloat16)
    return (hidden_out, c_new, k_new)
```

```python
import jax
import jax.numpy as jnp
from jax import lax
from jax.experimental import pallas as pl
from jax.experimental.pallas import tpu as pltpu
from jax.sharding import PartitionSpec as P

NOPE_DIM = 128
ROPE_DIM = 64
VALUE_DIM = 128
QK_DIM = NOPE_DIM + ROPE_DIM
EPSILON = 1e-6
ROUTE_SCALE = 2.5
ROPE_BASE = 10000.0
CAP_FACTOR = 2
MESH = pl.DeviceIdType.MESH
FF_TILE = 256
COL_TILE = 512
DEPTH_A = 3
DEPTH_B = 8
LANES = 128
SIB_LAG = 2


def rms_norm(vec, gain):
    vec = vec.astype(jnp.float32)
    scale = lax.rsqrt(jnp.mean(vec * vec, axis=-1, keepdims=True) + EPSILON)
    return vec * scale * gain.astype(jnp.float32)


def rotary(vec, positions):
    half = ROPE_DIM // 2
    freqs = ROPE_BASE ** (-jnp.arange(half).astype(jnp.float32) / half)
    angle = positions.astype(jnp.float32)[..., None] * freqs
    cosine = jnp.cos(angle)
    sine = jnp.sin(angle)
    first = vec[..., :half]
    second = vec[..., half:]
    return jnp.concatenate([first * cosine - second * sine, first * sine + second * cosine], axis=-1)


def attention_block(hidden, positions, ckv_cache, kpe_cache, attn_gain, w_dq, q_gain, w_uq, w_dkv, kv_gain, w_uk, w_uv, w_out):
    tokens = hidden.shape[0]
    kv_rank = w_uk.shape[0]
    heads = w_uk.shape[1] // NOPE_DIM
    cache_len = ckv_cache.shape[1]
    normed = rms_norm(hidden, attn_gain).astype(jnp.bfloat16)
    c_q = rms_norm(jnp.dot(normed, w_dq, preferred_element_type=jnp.float32), q_gain).astype(jnp.bfloat16)
    query = jnp.dot(c_q, w_uq, preferred_element_type=jnp.float32).astype(jnp.bfloat16).reshape(tokens, heads, QK_DIM)
    q_nope = query[:, :, :NOPE_DIM]
    q_rot = rotary(query[:, :, NOPE_DIM:].astype(jnp.float32), positions[:, None]).astype(jnp.bfloat16)
    kv_proj = jnp.dot(normed, w_dkv, preferred_element_type=jnp.float32)
    c_new = rms_norm(kv_proj[:, :kv_rank], kv_gain).astype(jnp.bfloat16)
    k_new = rotary(kv_proj[:, kv_rank:], positions).astype(jnp.bfloat16)
    q_abs = jnp.einsum('thn,chn->thc', q_nope, w_uk.reshape(kv_rank, heads, NOPE_DIM), preferred_element_type=jnp.float32).astype(jnp.bfloat16)
    scale = QK_DIM ** -0.5
    s_cache = (jnp.einsum('thc,tsc->ths', q_abs, ckv_cache, preferred_element_type=jnp.float32) + jnp.einsum('thr,tsr->ths', q_rot, kpe_cache, preferred_element_type=jnp.float32)) * scale
    valid = jnp.arange(cache_len)[None, None, :] < positions[:, None, None]
    s_cache = jnp.where(valid, s_cache, -1e30)
    s_self = (jnp.einsum('thc,tc->th', q_abs, c_new, preferred_element_type=jnp.float32) + jnp.einsum('thr,tr->th', q_rot, k_new, preferred_element_type=jnp.float32)) * scale
    peak = jnp.maximum(jnp.max(s_cache, axis=2), s_self)
    e_cache = jnp.exp(s_cache - peak[:, :, None])
    e_self = jnp.exp(s_self - peak)
    denominator = jnp.sum(e_cache, axis=2) + e_self
    p_cache = (e_cache / denominator[:, :, None]).astype(jnp.bfloat16)
    p_self = (e_self / denominator).astype(jnp.bfloat16)
    context = jnp.einsum('ths,tsc->thc', p_cache, ckv_cache, preferred_element_type=jnp.float32) + p_self.astype(jnp.float32)[:, :, None] * c_new.astype(jnp.float32)[:, None, :]
    heads_out = jnp.einsum('thc,chv->thv', context.astype(jnp.bfloat16), w_uv.reshape(kv_rank, heads, VALUE_DIM), preferred_element_type=jnp.float32).astype(jnp.bfloat16)
    attn_out = jnp.dot(heads_out.reshape(tokens, heads * VALUE_DIM), w_out, preferred_element_type=jnp.float32)
    x_mid = (hidden.astype(jnp.float32) + attn_out).astype(jnp.bfloat16)
    return x_mid, c_new, k_new


def gate_table(u_norm, topk_ids, w_router, capacity):
    experts = w_router.shape[1]
    tokens = u_norm.shape[0]
    gates = jax.nn.sigmoid(jnp.dot(u_norm, w_router, preferred_element_type=jnp.float32))
    hits = jnp.sum((topk_ids[:, :, None] == jnp.arange(experts)[None, None, :]).astype(jnp.float32), axis=1)
    total = jnp.sum(hits * gates, axis=1, keepdims=True)
    earlier = (jnp.arange(tokens)[:, None] > jnp.arange(tokens)[None, :]).astype(jnp.float32)
    before = jnp.dot(earlier, hits, preferred_element_type=jnp.float32)
    kept = jnp.where(before < capacity, hits, 0.0)
    table = kept * (ROUTE_SCALE * gates / total)
    return jnp.pad(table, ((0, 0), (0, LANES - experts)))


def moe_kernel(u_ref, xmid_ref, gw_ref, sg, su, sd, wg, wu, wd, out_ref,
               U, WT, wA, wB, acts, ACT, Pb, R1, RL, RX, RY, so,
               semA, semB, d_s, d_r, w_s, w_r, sib_s, sib_r, rl_s, rl_r, x_s, x_r, y_s, y_r):
    tokens, width = u_ref.shape
    ff = sg.shape[1]
    n_ff = ff // FF_TILE
    n_col = width // COL_TILE
    half = width // 2
    dp = lax.axis_index('dp')
    me = lax.axis_index('ep')
    core = lax.rem(me, 2)
    chip = me // 2
    cx = lax.rem(chip, 2)
    cy = chip // 2
    kX = cy * 2 + (1 - cx)
    kY = (1 - cy) * 2 + cx
    kD = (1 - cy) * 2 + (1 - cx)
    X = kX * 2 + core
    Y = kY * 2 + core
    D = kD * 2 + core
    sib = chip * 2 + (1 - core)

    def rows(dev):
        return pl.ds(pl.multiple_of(dev * tokens, tokens), tokens)

    def cols(j, size):
        return pl.ds(pl.multiple_of(j * size, size), size)

    def rcopy(src, dst, ss, rs, dev):
        return pltpu.make_async_remote_copy(src_ref=src, dst_ref=dst, send_sem=ss, recv_sem=rs,
                                            device_id=(dp, dev), device_id_type=MESH)

    def issueA(t):
        slot = lax.rem(t, DEPTH_A)

        @pl.when(t < n_ff)
        def _():
            pltpu.make_async_copy(sg.at[:, cols(t, FF_TILE)], wA.at[slot, :, 0:FF_TILE], semA.at[0, slot]).start()
            pltpu.make_async_copy(su.at[:, cols(t, FF_TILE)], wA.at[slot, :, FF_TILE:2 * FF_TILE], semA.at[1, slot]).start()

        @pl.when((t >= n_ff) & (t < 3 * n_ff))
        def _():
            e = t // n_ff - 1
            n = lax.rem(t, n_ff)
            pltpu.make_async_copy(wg.at[e, :, cols(n, FF_TILE)], wA.at[slot, :, 0:FF_TILE], semA.at[0, slot]).start()
            pltpu.make_async_copy(wu.at[e, :, cols(n, FF_TILE)], wA.at[slot, :, FF_TILE:2 * FF_TILE], semA.at[1, slot]).start()

    def waitA(t):
        slot = lax.rem(t, DEPTH_A)
        pltpu.make_async_copy(sg.at[:, 0:FF_TILE], wA.at[slot, :, 0:FF_TILE], semA.at[0, slot]).wait()
        pltpu.make_async_copy(su.at[:, 0:FF_TILE], wA.at[slot, :, FF_TILE:2 * FF_TILE], semA.at[1, slot]).wait()

    def issueB(b):
        slot = lax.rem(b, DEPTH_B)

        @pl.when(b < 2 * n_col)
        def _():
            pltpu.make_async_copy(wd.at[lax.rem(b, 2), :, cols(b // 2, COL_TILE)], wB.at[slot], semB.at[slot]).start()

        @pl.when((b >= 2 * n_col) & (b < 3 * n_col))
        def _():
            pltpu.make_async_copy(sd.at[:, cols(b - 2 * n_col, COL_TILE)], wB.at[slot], semB.at[slot]).start()

    def waitB(b):
        slot = lax.rem(b, DEPTH_B)
        pltpu.make_async_copy(sd.at[:, 0:COL_TILE], wB.at[slot], semB.at[slot]).wait()

    for t in range(DEPTH_A):
        issueA(jnp.int32(t))

    barrier = pltpu.get_barrier_semaphore()
    for k in range(1, 8):
        pl.semaphore_signal(barrier, inc=1, device_id=(dp, lax.rem(me + k, 8)), device_id_type=MESH)
    pl.semaphore_wait(barrier, 7)

    h0 = slice(0, half)
    h1 = slice(half, width)
    own = rows(me)
    rX, rY, rD = rows(X), rows(Y), rows(D)
    toX0 = rcopy(u_ref.at[:, h0], U.at[own, h0], d_s.at[0], d_r.at[0], X)
    toY1 = rcopy(u_ref.at[:, h1], U.at[own, h1], d_s.at[1], d_r.at[1], Y)
    toX1 = rcopy(u_ref.at[:, h1], U.at[own, h1], d_s.at[2], d_r.at[2], X)
    toY0 = rcopy(u_ref.at[:, h0], U.at[own, h0], d_s.at[3], d_r.at[3], Y)
    toS = rcopy(u_ref, U.at[own, :], d_s.at[4], d_r.at[4], sib)
    toX0.start()
    toY1.start()
    toX1.start()
    toY0.start()
    toS.start()
    for k in range(1, 8):
        rcopy(gw_ref, WT.at[own, :], w_s.at[k], w_r.at[k], lax.rem(me + k, 8)).start()
    WT[own, :] = gw_ref[...]
    U[own, :] = u_ref[...]

    fromX0 = rcopy(u_ref.at[:, h0], U.at[rX, h0], d_s.at[0], d_r.at[0], X)
    fromY1 = rcopy(u_ref.at[:, h1], U.at[rY, h1], d_s.at[1], d_r.at[1], Y)
    fromX1 = rcopy(u_ref.at[:, h1], U.at[rX, h1], d_s.at[2], d_r.at[2], X)
    fromY0 = rcopy(u_ref.at[:, h0], U.at[rY, h0], d_s.at[3], d_r.at[3], Y)
    relY = rcopy(U.at[rX, h0], U.at[rX, h0], d_s.at[5], d_r.at[5], Y)
    relX = rcopy(U.at[rY, h1], U.at[rY, h1], d_s.at[6], d_r.at[6], X)
    fromD0 = rcopy(U.at[rX, h0], U.at[rD, h0], d_s.at[5], d_r.at[5], Y)
    fromD1 = rcopy(U.at[rY, h1], U.at[rD, h1], d_s.at[6], d_r.at[6], X)
    sX = rcopy(U.at[rX, :], U.at[rX, :], d_s.at[7], d_r.at[7], sib)
    sY = rcopy(U.at[rY, :], U.at[rY, :], d_s.at[8], d_r.at[8], sib)
    sD = rcopy(U.at[rD, :], U.at[rD, :], d_s.at[9], d_r.at[9], sib)

    def sib_rows(k):
        return rows(k * 2 + (1 - core))

    def gated(both):
        g = both[:, 0:FF_TILE]
        return (g * jax.nn.sigmoid(g) * both[:, FF_TILE:2 * FF_TILE]).astype(jnp.bfloat16)

    def shared_up_step(t, carry):
        waitA(t)
        both = jnp.dot(u_ref[...], wA[lax.rem(t, DEPTH_A)], preferred_element_type=jnp.float32)
        acts[:, cols(t, FF_TILE)] = gated(both)
        issueA(t + DEPTH_A)

        @pl.when(t == 2)
        def _():
            fromX0.wait_recv()
            relY.start()
            fromY1.wait_recv()
            relX.start()

        @pl.when(t == 5)
        def _():
            fromX1.wait_recv()
            sX.start()
            fromY0.wait_recv()
            sY.start()
            for b in range(DEPTH_B):
                issueB(jnp.int32(b))
        return carry

    lax.fori_loop(0, n_ff, shared_up_step, 0)

    fromD0.wait_recv()
    fromD1.wait_recv()
    sD.start()
    rcopy(u_ref, U.at[sib_rows(chip), :], d_s.at[4], d_r.at[4], sib).wait_recv()
    rcopy(U.at[rX, :], U.at[sib_rows(kX), :], d_s.at[7], d_r.at[7], sib).wait_recv()
    rcopy(U.at[rY, :], U.at[sib_rows(kY), :], d_s.at[8], d_r.at[8], sib).wait_recv()
    rcopy(U.at[rD, :], U.at[sib_rows(kD), :], d_s.at[9], d_r.at[9], sib).wait_recv()
    for k in range(1, 8):
        rcopy(gw_ref, WT.at[rows(lax.rem(me + 8 - k, 8)), :], w_s.at[k], w_r.at[k], lax.rem(me + k, 8)).wait_recv()

    def routed_up_step(t, carry):
        waitA(t)
        both = jnp.dot(U[...], wA[lax.rem(t, DEPTH_A)], preferred_element_type=jnp.float32)
        ACT[t // n_ff - 1, :, cols(lax.rem(t, n_ff), FF_TILE)] = gated(both)
        issueA(t + DEPTH_A)
        return carry

    lax.fori_loop(n_ff, 3 * n_ff, routed_up_step, 0)

    for cp in (toX0, toY1, toX1, toY0, toS, relY, relX, sX, sY, sD):
        cp.wait_send()
    for k in range(1, 8):
        rcopy(gw_ref, WT.at[own, :], w_s.at[k], w_r.at[k], lax.rem(me + k, 8)).wait_send()

    lane = lax.broadcasted_iota(jnp.int32, WT.shape, 1)
    w0 = jnp.sum(jnp.where(lane == 2 * me, WT[...], 0.0), axis=1, keepdims=True)
    w1 = jnp.sum(jnp.where(lane == 2 * me + 1, WT[...], 0.0), axis=1, keepdims=True)

    def to_sib(j):
        return rcopy(Pb.at[1 - core, :, :, cols(j, COL_TILE)], R1.at[:, :, cols(j, COL_TILE)], sib_s.at[j], sib_r.at[j], sib)

    def first_leg(j, dev):
        return rcopy(Pb.at[core, kD, :, cols(j, COL_TILE)], RL.at[:, cols(j, COL_TILE)], rl_s.at[j], rl_r.at[j], dev)

    def last_x(j):
        return rcopy(Pb.at[core, kX, :, cols(j, COL_TILE)], RX.at[:, cols(j, COL_TILE)], x_s.at[j], x_r.at[j], X)

    def last_y(j):
        return rcopy(Pb.at[core, kY, :, cols(j, COL_TILE)], RY.at[:, cols(j, COL_TILE)], y_s.at[j], y_r.at[j], Y)

    def chip_sum(j):
        to_sib(j).wait_recv()
        Pb[core, :, :, cols(j, COL_TILE)] = Pb[core, :, :, cols(j, COL_TILE)] + R1[:, :, cols(j, COL_TILE)]
        odd = lax.rem(j, 2)

        @pl.when(odd == 0)
        def _():
            first_leg(j, X).start()
            last_x(j).start()

        @pl.when(odd == 1)
        def _():
            first_leg(j, Y).start()
            last_y(j).start()

    def relay(j):
        odd = lax.rem(j, 2)

        @pl.when(odd == 0)
        def _():
            first_leg(j, X).wait_recv()
            Pb[core, kY, :, cols(j, COL_TILE)] = Pb[core, kY, :, cols(j, COL_TILE)] + RL[:, cols(j, COL_TILE)]
            last_y(j).start()

        @pl.when(odd == 1)
        def _():
            first_leg(j, Y).wait_recv()
            Pb[core, kX, :, cols(j, COL_TILE)] = Pb[core, kX, :, cols(j, COL_TILE)] + RL[:, cols(j, COL_TILE)]
            last_x(j).start()

    def down_step(j, carry):
        waitB(2 * j)
        waitB(2 * j + 1)
        e0 = jnp.dot(ACT[0], wB[lax.rem(2 * j, DEPTH_B)], preferred_element_type=jnp.float32).astype(jnp.bfloat16)
        e1 = jnp.dot(ACT[1], wB[lax.rem(2 * j + 1, DEPTH_B)], preferred_element_type=jnp.float32).astype(jnp.bfloat16)
        part = w0 * e0.astype(jnp.float32) + w1 * e1.astype(jnp.float32)
        for k in range(4):
            for c in range(2):
                r = (2 * k + c) * tokens
                Pb[c, k, :, cols(j, COL_TILE)] = part[r:r + tokens]
        to_sib(j).start()
        issueB(2 * j + DEPTH_B)
        issueB(2 * j + 1 + DEPTH_B)

        @pl.when(j >= SIB_LAG)
        def _():
            chip_sum(j - SIB_LAG)

        @pl.when((j >= 5) & (lax.rem(j, 2) == 1))
        def _():
            relay((j - 5) // 2)
        return carry

    lax.fori_loop(0, n_col, down_step, 0)
    for j in range(n_col - SIB_LAG, n_col):
        chip_sum(jnp.int32(j))
    relayed = (n_col - 5 + 1) // 2

    def shared_down_step(j, carry):
        b = 2 * n_col + j
        waitB(b)
        so[:, cols(j, COL_TILE)] = jnp.dot(acts[...], wB[lax.rem(b, DEPTH_B)], preferred_element_type=jnp.float32).astype(jnp.bfloat16)
        issueB(b + DEPTH_B)

        @pl.when(lax.rem(j, 2) == 0)
        def _():
            relay(relayed + j // 2)
        return carry

    lax.fori_loop(0, n_col, shared_down_step, 0)
    for j in range(relayed + (n_col + 1) // 2, n_col):
        relay(jnp.int32(j))

    def finish(j, carry):
        last_x(j).wait_recv()
        last_y(j).wait_recv()
        s = cols(j, COL_TILE)
        routed = Pb[core, chip, :, s] + RX[:, s] + RY[:, s]
        out_ref[:, s] = (xmid_ref[:, s].astype(jnp.float32) + routed + so[:, s].astype(jnp.float32)).astype(jnp.bfloat16)
        to_sib(j).wait_send()
        first_leg(j, X).wait_send()
        last_x(j).wait_send()
        last_y(j).wait_send()
        return carry

    lax.fori_loop(0, n_col, finish, 0)


def moe_call(u_norm, x_mid, table, shared_gate, shared_up, shared_down, w_gate, w_up, w_down):
    tokens, width = u_norm.shape
    ff = shared_gate.shape[1]
    total = 8 * tokens
    n_col = width // COL_TILE
    vmem = pl.BlockSpec(memory_space=pltpu.VMEM)
    hbm = pl.BlockSpec(memory_space=pl.ANY)
    dma = pltpu.SemaphoreType.DMA
    bf, f4 = jnp.bfloat16, jnp.float32
    return pl.pallas_call(
        moe_kernel,
        out_shape=jax.ShapeDtypeStruct((tokens, width), bf),
        in_specs=[vmem] * 3 + [hbm] * 6,
        out_specs=vmem,
        scratch_shapes=[
            pltpu.VMEM((total, width), bf),
            pltpu.VMEM((total, LANES), f4),
            pltpu.VMEM((DEPTH_A, width, 2 * FF_TILE), bf),
            pltpu.VMEM((DEPTH_B, ff, COL_TILE), bf),
            pltpu.VMEM((tokens, ff), bf),
            pltpu.VMEM((2, total, ff), bf),
            pltpu.VMEM((2, 4, tokens, width), f4),
            pltpu.VMEM((4, tokens, width), f4),
            pltpu.VMEM((tokens, width), f4),
            pltpu.VMEM((tokens, width), f4),
            pltpu.VMEM((tokens, width), f4),
            pltpu.VMEM((tokens, width), bf),
            dma((2, DEPTH_A)), dma((DEPTH_B,)), dma((10,)), dma((10,)), dma((8,)), dma((8,)),
        ] + [dma((n_col,))] * 8,
        compiler_params=pltpu.CompilerParams(collective_id=0, has_side_effects=True, vmem_limit_bytes=67043328),
        name='moe_exchange',
    )(u_norm, x_mid, table, shared_gate, shared_up, shared_down, w_gate, w_up, w_down)


def solution(mesh):
    batch = P(('dp', 'ep'))
    whole = P()
    by_expert = P('ep')

    def local_step(hidden, positions, ckv_cache, kpe_cache, topk_ids, attn_gain, w_dq, q_gain, w_uq, w_dkv, kv_gain, w_uk, w_uv, w_out, ffn_gain, w_router, w_gate, w_up, w_down, shared_gate, shared_up, shared_down):
        x_mid, c_new, k_new = attention_block(hidden, positions, ckv_cache, kpe_cache, attn_gain, w_dq, q_gain, w_uq, w_dkv, kv_gain, w_uk, w_uv, w_out)
        u_norm = rms_norm(x_mid, ffn_gain).astype(jnp.bfloat16)
        tokens = u_norm.shape[0]
        experts = w_router.shape[1]
        capacity = (CAP_FACTOR * tokens * topk_ids.shape[1] + experts - 1) // experts
        table = gate_table(u_norm, topk_ids, w_router, capacity)
        hidden_out = moe_call(u_norm, x_mid, table, shared_gate, shared_up, shared_down, w_gate, w_up, w_down)
        return hidden_out, c_new, k_new

    in_specs = (batch,) * 5 + (whole,) * 11 + (by_expert,) * 3 + (whole,) * 3
    return jax.shard_map(local_step, mesh=mesh, in_specs=in_specs, out_specs=(batch, batch, batch), check_vma=False)
```

```python
import jax
import jax.numpy as jnp
import numpy as np
from jax import lax
from jax.experimental import pallas as pl
from jax.experimental.pallas import tpu as pltpu
from jax.sharding import PartitionSpec as P

NOPE_DIM = 128
ROPE_DIM = 64
VALUE_DIM = 128
QK_DIM = NOPE_DIM + ROPE_DIM
EPSILON = 1e-6
ROUTE_SCALE = 2.5
ROPE_BASE = 10000.0
CAP_FACTOR = 2
MESH = pl.DeviceIdType.MESH
HEADS = 16
CACHE = 64
FF_TILE = 256
COL_TILE = 512
Q_TILE = 2 * QK_DIM
GROUP = 1024
KV_ROWS = 1024
DEPTH_A = 3
DEPTH_B = 7
LANES = 128
SCALE_LANE = 64
SIB_LAG = 2
SIB_SLOTS = 4
EARLY = 5
SUB = 8
BF = jnp.bfloat16
F4 = jnp.float32


def layer_kernel(pos_ref, topk_ref, freq_ref, ag_ref, qg_ref, kg_ref, fg_ref,
                 hidden, ckv, kpe, dq, uq, dkv, uk, uv, wo, router, sg, su, sd, wg, wu, wd,
                 out_ref, cnew_ref, knew_ref,
                 U, WT, wA, wB, wD, wR, kp, kvs, hid, xm, cq, QN, QA, QR, CTX, O, acts, ACT, Pm, Ps, R1, RL, RX, RY,
                 semA, semB, semD, semM, px_s, px_r, py_s, py_r, pr_s, pr_r, d_s, d_r, w_s, w_r,
                 sib_s, sib_r, rl_s, rl_r, x_s, x_r, y_s, y_r):
    tokens, width = hid.shape
    ff = sg.shape[1]
    rank = uk.shape[0]
    q_rank = cq.shape[1]
    n_ff = ff // FF_TILE
    n_col = width // COL_TILE
    n_grp = width // GROUP
    n_q = uq.shape[1] // Q_TILE
    n_dq = q_rank // COL_TILE
    dp = lax.axis_index('dp')
    me = lax.axis_index('ep')
    core = lax.rem(me, 2)
    chip = me // 2
    cx = lax.rem(chip, 2)
    cy = chip // 2
    kX = cy * 2 + (1 - cx)
    kY = (1 - cy) * 2 + cx
    kD = (1 - cy) * 2 + (1 - cx)
    X = kX * 2 + core
    Y = kY * 2 + core
    sib = chip * 2 + (1 - core)

    def rows(block):
        return pl.ds(pl.multiple_of(block * tokens, tokens), tokens)

    def cols(j, size):
        return pl.ds(pl.multiple_of(j * size, size), size)

    def copy(src, dst, sem):
        return pltpu.make_async_copy(src, dst, sem)

    def rcopy(src, dst, ss, rs, dev):
        return pltpu.make_async_remote_copy(src_ref=src, dst_ref=dst, send_sem=ss, recv_sem=rs,
                                            device_id=(dp, dev), device_id_type=MESH)

    def dot(a, b):
        return jnp.dot(a, b, preferred_element_type=F4)

    def dot_t(a, b):
        return lax.dot_general(a, b, (((1,), (1,)), ((), ())), preferred_element_type=F4)

    A_S0 = n_dq
    A_R = A_S0 + EARLY
    A_S1 = A_R + 2 * n_ff
    A_END = A_S1 + n_ff - EARLY

    def issueA(t):
        slot = lax.rem(t, DEPTH_A)

        def pair(left, right):
            copy(left, wA.at[slot, :, 0:FF_TILE], semA.at[0, slot]).start()
            copy(right, wA.at[slot, :, FF_TILE:2 * FF_TILE], semA.at[1, slot]).start()

        @pl.when(t < n_dq)
        def _():
            copy(dq.at[:, cols(t, COL_TILE)], wA.at[slot], semA.at[0, slot]).start()

        @pl.when((t >= A_S0) & (t < A_R))
        def _():
            n = t - A_S0
            pair(sg.at[:, cols(n, FF_TILE)], su.at[:, cols(n, FF_TILE)])

        @pl.when((t >= A_R) & (t < A_S1))
        def _():
            e = (t - A_R) // n_ff
            n = lax.rem(t - A_R, n_ff)
            pair(wg.at[e, :, cols(n, FF_TILE)], wu.at[e, :, cols(n, FF_TILE)])

        @pl.when((t >= A_S1) & (t < A_END))
        def _():
            n = t - A_S1 + EARLY
            pair(sg.at[:, cols(n, FF_TILE)], su.at[:, cols(n, FF_TILE)])

    def wait_whole(t):
        slot = lax.rem(t, DEPTH_A)
        copy(dq.at[:, 0:COL_TILE], wA.at[slot], semA.at[0, slot]).wait()

    def wait_pair(t):
        slot = lax.rem(t, DEPTH_A)
        copy(sg.at[:, 0:FF_TILE], wA.at[slot, :, 0:FF_TILE], semA.at[0, slot]).wait()
        copy(su.at[:, 0:FF_TILE], wA.at[slot, :, FF_TILE:2 * FF_TILE], semA.at[1, slot]).wait()

    B_UK = n_q
    B_CKV = n_q + 1
    B_UV = n_q + 2
    B_O = n_q + 3
    B_D = B_O + n_col
    B_S = B_D + 2 * n_col
    B_END = B_S + n_col

    def issueB(b):
        slot = lax.rem(b, DEPTH_B)

        def blocks(src):
            for q in range(4):
                copy(src.at[:, q * COL_TILE:(q + 1) * COL_TILE], wB.at[slot, q * rank:(q + 1) * rank, :], semB.at[slot]).start()

        @pl.when(b < n_q)
        def _():
            copy(uq.at[:, cols(b, Q_TILE)], wB.at[slot, 0:q_rank, 0:Q_TILE], semB.at[slot]).start()

        @pl.when(b == B_UK)
        def _():
            blocks(uk)

        @pl.when(b == B_CKV)
        def _():
            copy(ckv, wB.at[slot], semB.at[slot]).start()

        @pl.when(b == B_UV)
        def _():
            blocks(uv)

        @pl.when((b >= B_O) & (b < B_D))
        def _():
            copy(wo.at[:, cols(b - B_O, COL_TILE)], wB.at[slot], semB.at[slot]).start()

        @pl.when((b >= B_D) & (b < B_S))
        def _():
            copy(wd.at[lax.rem(b - B_D, 2), :, cols((b - B_D) // 2, COL_TILE)], wB.at[slot], semB.at[slot]).start()

        @pl.when((b >= B_S) & (b < B_END))
        def _():
            copy(sd.at[:, cols(b - B_S, COL_TILE)], wB.at[slot], semB.at[slot]).start()

    def waitB(b):
        slot = lax.rem(b, DEPTH_B)
        copy(sd.at[:, 0:COL_TILE], wB.at[slot], semB.at[slot]).wait()

    n_kv = width // KV_ROWS

    def kv_copy(c):
        slot = lax.rem(c, 2)
        return copy(dkv.at[:, cols(c, KV_ROWS)], wD.at[slot], semD.at[slot])

    copy(hidden, hid, semM.at[0]).start()
    for t in range(DEPTH_A):
        issueA(jnp.int32(t))
    for b in range(DEPTH_B):
        issueB(jnp.int32(b))
    for c in range(2):
        kv_copy(jnp.int32(c)).start()
    copy(kpe, kp, semM.at[1]).start()
    copy(router, wR, semM.at[2]).start()

    barrier = pltpu.get_barrier_semaphore()
    for k in range(1, 8):
        pl.semaphore_signal(barrier, inc=1, device_id=(dp, lax.rem(me + k, 8)), device_id_type=MESH)

    row_id = lax.broadcasted_iota(jnp.int32, (tokens, ROPE_DIM), 0)
    posv = jnp.zeros((tokens, ROPE_DIM), jnp.int32)
    for t in range(tokens):
        posv = jnp.where(row_id == t, pos_ref[t], posv)
    angle = posv.astype(F4) * freq_ref[0:1, 0:ROPE_DIM]
    cosine = jnp.cos(angle)
    sine = jnp.sin(angle) * freq_ref[1:2, 0:ROPE_DIM]

    def rotate(v):
        other = jnp.concatenate([v[:, ROPE_DIM // 2:], v[:, :ROPE_DIM // 2]], axis=1)
        return v * cosine + other * sine

    def gain(ref):
        return ref[...].astype(F4).reshape(1, -1)

    def rms(v, gain):
        scale = lax.rsqrt(jnp.mean(v * v, axis=-1, keepdims=True) + EPSILON)
        return v * scale * gain

    copy(hidden, hid, semM.at[0]).wait()
    own = rows(chip)
    U[own, :] = rms(hid[...].astype(F4), gain(ag_ref)).astype(BF)

    def dq_step(t, carry):
        wait_whole(t)
        cq[:, cols(t, COL_TILE)] = dot(U[own, :], wA[lax.rem(t, DEPTH_A)])
        issueA(t + DEPTH_A)
        return carry

    lax.fori_loop(0, n_dq, dq_step, 0)
    kvs[...] = jnp.zeros_like(kvs)
    c_q = rms(cq[...], gain(qg_ref)).astype(BF)
    cq[...] = c_q.astype(F4)

    def put(ref, h, val):
        for g in range(tokens // SUB):
            ref[g, h] = val[g * SUB:(g + 1) * SUB]

    def uq_step(b, carry):
        slot = lax.rem(b, DEPTH_B)
        copy(uq.at[:, 0:Q_TILE], wB.at[slot, 0:q_rank, 0:Q_TILE], semB.at[slot]).wait()
        q2 = dot(cq[...].astype(BF), wB[slot, 0:q_rank, 0:Q_TILE]).astype(BF).astype(F4)
        issueB(b + DEPTH_B)
        for i in range(2):
            base = i * QK_DIM
            QN[2 * b + i] = q2[:, base:base + NOPE_DIM].astype(BF)
            put(QR, 2 * b + i, rotate(q2[:, base + NOPE_DIM:base + QK_DIM]).astype(BF).astype(F4))

        @pl.when(b < n_kv)
        def _():
            kv_copy(b).wait()
            kvs[...] = kvs[...] + dot_t(U[own, cols(b, KV_ROWS)], wD[lax.rem(b, 2)])

            @pl.when(b + 2 < n_kv)
            def _():
                kv_copy(b + 2).start()
        return carry

    lax.fori_loop(0, n_q, uq_step, 0)

    cnew_ref[...] = rms(kvs[:, 0:rank], gain(kg_ref)).astype(BF)
    knew_ref[...] = rotate(kvs[:, rank:rank + ROPE_DIM]).astype(BF)

    waitB(B_UK)
    slot_uk = B_UK % DEPTH_B

    for h in range(HEADS):
        w_h = wB[slot_uk, (h // 4) * rank:(h // 4 + 1) * rank, (h % 4) * NOPE_DIM:(h % 4 + 1) * NOPE_DIM]
        put(QA, h, dot_t(QN[h], w_h).astype(BF).astype(F4))
    issueB(jnp.int32(B_UK + DEPTH_B))

    waitB(B_CKV)
    slot_ckv = B_CKV % DEPTH_B
    copy(kpe, kp, semM.at[1]).wait()
    span = SUB * CACHE
    scale = QK_DIM ** -0.5
    lane = lax.broadcasted_iota(jnp.int32, (SUB, span), 1)
    tok = lax.broadcasted_iota(jnp.int32, (SUB, span), 0)
    for g in range(tokens // SUB):
        keys = wB[slot_ckv, g * span:(g + 1) * span, :]
        qa = QA[g]
        qr = QR[g]
        cn = cnew_ref[g * SUB:(g + 1) * SUB, :].astype(F4)
        kn = knew_ref[g * SUB:(g + 1) * SUB, :].astype(F4)
        s = dot_t(qa.reshape(HEADS * SUB, rank).astype(BF), keys)
        s = s + dot_t(qr.reshape(HEADS * SUB, ROPE_DIM).astype(BF), kp[g * span:(g + 1) * span, :])
        s = s.reshape(HEADS, SUB, span) * scale
        limit = posv[g * SUB:(g + 1) * SUB, 0:1]
        valid = (lane >= tok * CACHE) & (lane < tok * CACHE + limit)
        s = jnp.where(valid[None], s, -1e30)
        s_self = (jnp.sum(qa * cn[None], axis=2, keepdims=True) + jnp.sum(qr * kn[None], axis=2, keepdims=True)) * scale
        peak = jnp.maximum(jnp.max(s, axis=2, keepdims=True), s_self)
        e = jnp.where(valid[None], jnp.exp(s - peak), 0.0)
        e_self = jnp.exp(s_self - peak)
        denom = jnp.sum(e, axis=2, keepdims=True) + e_self
        p = (e / denom).astype(BF)
        p_self = (e_self / denom).astype(BF).astype(F4)
        ctx = dot(p.reshape(HEADS * SUB, span), keys).reshape(HEADS, SUB, rank) + p_self * cn[None]
        CTX[g] = ctx.astype(BF).astype(F4)
    issueB(jnp.int32(B_CKV + DEPTH_B))

    waitB(B_UV)
    slot_uv = B_UV % DEPTH_B
    for h in range(HEADS):
        w_h = wB[slot_uv, (h // 4) * rank:(h // 4 + 1) * rank, (h % 4) * VALUE_DIM:(h % 4 + 1) * VALUE_DIM]
        O[:, h * VALUE_DIM:(h + 1) * VALUE_DIM] = dot(CTX[:, h].reshape(tokens, rank).astype(BF), w_h).astype(BF)
    issueB(jnp.int32(B_UV + DEPTH_B))

    pl.semaphore_wait(barrier, 7)

    def grp_x(p, block):
        return rcopy(xm.at[:, cols(p, GROUP)], U.at[rows(block), cols(p, GROUP)], px_s.at[p], px_r.at[p], X)

    def grp_y(p, block):
        return rcopy(xm.at[:, cols(p, GROUP)], U.at[rows(block), cols(p, GROUP)], py_s.at[p], py_r.at[p], Y)

    def pass_y(p, block):
        return rcopy(U.at[rows(kX), cols(p, GROUP)], U.at[rows(block), cols(p, GROUP)], pr_s.at[p], pr_r.at[p], Y)

    def pass_x(p, block):
        return rcopy(U.at[rows(kY), cols(p, GROUP)], U.at[rows(block), cols(p, GROUP)], pr_s.at[p], pr_r.at[p], X)

    def forward(p):
        grp_x(p, kX).wait_recv()
        grp_y(p, kY).wait_recv()
        odd = lax.rem(p, 2)

        @pl.when(odd == 0)
        def _():
            pass_y(p, kX).start()

        @pl.when(odd == 1)
        def _():
            pass_x(p, kY).start()

    def out_step(j, carry):
        b = B_O + j
        waitB(b)
        att = dot(O[...], wB[lax.rem(b, DEPTH_B)])
        xm[:, cols(j, COL_TILE)] = (hid[:, cols(j, COL_TILE)].astype(F4) + att).astype(BF)
        issueB(b + DEPTH_B)

        @pl.when(lax.rem(j, 2) == 1)
        def _():
            p = j // 2
            grp_x(p, chip).start()
            grp_y(p, chip).start()

            @pl.when(p >= 3)
            def _():
                forward(p - 3)
        return carry

    lax.fori_loop(0, n_col, out_step, 0)
    toS = rcopy(xm, U.at[rows(4 + chip), :], d_s.at[0], d_r.at[0], sib)
    toS.start()

    xf = xm[...].astype(F4)
    row_scale = lax.rsqrt(jnp.mean(xf * xf, axis=-1, keepdims=True) + EPSILON)
    u_own = (xf * row_scale * gain(fg_ref)).astype(BF)
    U[own, :] = u_own
    copy(router, wR, semM.at[2]).wait()
    experts = router.shape[0]
    capacity = (CAP_FACTOR * tokens * topk_ref.shape[0] + experts - 1) // experts
    gates = jax.nn.sigmoid(dot_t(U[own, :], wR[...]))
    eid = lax.broadcasted_iota(jnp.int32, (experts, tokens), 0)
    picks = jnp.zeros((experts, tokens), F4)
    for k in range(topk_ref.shape[0]):
        picks = picks + jnp.where(topk_ref[k:k + 1, :] == eid, 1.0, 0.0)
    picks = picks.astype(BF)
    here = lax.broadcasted_iota(jnp.int32, (tokens, tokens), 0)
    there = lax.broadcasted_iota(jnp.int32, (tokens, tokens), 1)
    hits = dot_t(jnp.where(here == there, 1.0, 0.0).astype(BF), picks)
    before = dot_t(jnp.where(here > there, 1.0, 0.0).astype(BF), picks)
    total = jnp.sum(hits * gates, axis=1, keepdims=True)
    table = jnp.where(before < capacity, hits, 0.0) * (ROUTE_SCALE * gates / total)
    WT[own, 0:experts] = table
    WT[own, SCALE_LANE:LANES] = jnp.broadcast_to(row_scale, (tokens, LANES - SCALE_LANE))

    def table_to(k):
        dev = lax.rem(me + k, 8)
        block = chip + 4 * lax.rem(core + dev, 2)
        return rcopy(WT.at[own, :], WT.at[rows(block), :], w_s.at[k], w_r.at[k], dev)

    def table_from(k):
        dev = lax.rem(me + 8 - k, 8)
        block = dev // 2 + 4 * lax.rem(core + dev, 2)
        return rcopy(WT.at[rows(block), :], WT.at[rows(block), :], w_s.at[k], w_r.at[k], dev)

    for k in range(1, 8):
        table_to(k).start()

    def gated(both):
        g = both[:, 0:FF_TILE]
        return (g * jax.nn.sigmoid(g) * both[:, FF_TILE:2 * FF_TILE]).astype(BF)

    def to_twin(i, k):
        return rcopy(U.at[rows(k), :], U.at[rows(4 + k), :], d_s.at[i], d_r.at[i], sib)

    def shared_early(n, carry):
        t = A_S0 + n
        wait_pair(t)
        acts[:, cols(n, FF_TILE)] = gated(dot(U[own, :], wA[lax.rem(t, DEPTH_A)]))
        issueA(t + DEPTH_A)

        @pl.when(n < 3)
        def _():
            forward(n_grp - 3 + n)

        @pl.when(n == 3)
        def _():
            to_twin(1, kX).start()
            to_twin(2, kY).start()
        return carry

    lax.fori_loop(0, EARLY, shared_early, 0)

    for p in range(n_grp):
        if p % 2 == 0:
            pass_y(p, kD).wait_recv()
        else:
            pass_x(p, kD).wait_recv()
    to_twin(3, kD).start()
    rcopy(xm, U.at[rows(4 + chip), :], d_s.at[0], d_r.at[0], sib).wait_recv()
    for i, k in ((1, kX), (2, kY), (3, kD)):
        rcopy(U.at[rows(k), :], U.at[rows(4 + k), :], d_s.at[i], d_r.at[i], sib).wait_recv()
    toS.wait_send()
    for i, k in ((1, kX), (2, kY), (3, kD)):
        to_twin(i, k).wait_send()
    for p in range(n_grp):
        grp_x(p, chip).wait_send()
        grp_y(p, chip).wait_send()
        if p % 2 == 0:
            pass_y(p, kX).wait_send()
        else:
            pass_x(p, kY).wait_send()
    for k in range(1, 8):
        table_from(k).wait_recv()

    def normalise(i, carry):
        block = lax.rem(chip + i, 8)
        r = rows(block)
        U[r, :] = (U[r, :].astype(F4) * WT[r, SCALE_LANE:SCALE_LANE + 1] * gain(fg_ref)).astype(BF)
        return carry

    lax.fori_loop(1, 8, normalise, 0)

    def routed_up_step(i, carry):
        t = A_R + i
        wait_pair(t)
        both = dot(U[...], wA[lax.rem(t, DEPTH_A)])
        ACT[i // n_ff, :, cols(lax.rem(i, n_ff), FF_TILE)] = gated(both)
        issueA(t + DEPTH_A)
        return carry

    lax.fori_loop(0, 2 * n_ff, routed_up_step, 0)

    for k in range(1, 8):
        table_to(k).wait_send()

    lane_id = lax.broadcasted_iota(jnp.int32, WT.shape, 1)
    w0 = jnp.sum(jnp.where(lane_id == 2 * me, WT[...], 0.0), axis=1, keepdims=True)
    w1 = jnp.sum(jnp.where(lane_id == 2 * me + 1, WT[...], 0.0), axis=1, keepdims=True)

    def to_sib(j):
        return rcopy(Ps.at[lax.rem(j, SIB_SLOTS)], R1.at[:, :, cols(j, COL_TILE)], sib_s.at[j], sib_r.at[j], sib)

    def first_leg(j, dev):
        return rcopy(Pm.at[kD, :, cols(j, COL_TILE)], RL.at[:, cols(j, COL_TILE)], rl_s.at[j], rl_r.at[j], dev)

    def last_x(j):
        return rcopy(Pm.at[kX, :, cols(j, COL_TILE)], RX.at[:, cols(j, COL_TILE)], x_s.at[j], x_r.at[j], X)

    def last_y(j):
        return rcopy(Pm.at[kY, :, cols(j, COL_TILE)], RY.at[:, cols(j, COL_TILE)], y_s.at[j], y_r.at[j], Y)

    def chip_sum(j):
        to_sib(j).wait_recv()
        Pm[:, :, cols(j, COL_TILE)] = Pm[:, :, cols(j, COL_TILE)] + R1[:, :, cols(j, COL_TILE)]
        odd = lax.rem(j, 2)

        @pl.when(odd == 0)
        def _():
            first_leg(j, X).start()
            last_x(j).start()

        @pl.when(odd == 1)
        def _():
            first_leg(j, Y).start()
            last_y(j).start()

    def relay(j):
        odd = lax.rem(j, 2)

        @pl.when(odd == 0)
        def _():
            first_leg(j, X).wait_recv()
            Pm[kY, :, cols(j, COL_TILE)] = Pm[kY, :, cols(j, COL_TILE)] + RL[:, cols(j, COL_TILE)]
            last_y(j).start()

        @pl.when(odd == 1)
        def _():
            first_leg(j, Y).wait_recv()
            Pm[kX, :, cols(j, COL_TILE)] = Pm[kX, :, cols(j, COL_TILE)] + RL[:, cols(j, COL_TILE)]
            last_x(j).start()

    def down_step(j, carry):
        b = B_D + 2 * j
        waitB(b)
        waitB(b + 1)
        e0 = dot(ACT[0], wB[lax.rem(b, DEPTH_B)]).astype(BF)
        e1 = dot(ACT[1], wB[lax.rem(b + 1, DEPTH_B)]).astype(BF)

        @pl.when(j >= SIB_SLOTS)
        def _():
            to_sib(j - SIB_SLOTS).wait_send()

        part = w0 * e0.astype(F4) + w1 * e1.astype(F4)
        Pm[:, :, cols(j, COL_TILE)] = part[0:4 * tokens].reshape(4, tokens, COL_TILE)
        Ps[lax.rem(j, SIB_SLOTS)] = part[4 * tokens:8 * tokens].reshape(4, tokens, COL_TILE)
        to_sib(j).start()
        issueB(b + DEPTH_B)
        issueB(b + 1 + DEPTH_B)

        @pl.when(j >= SIB_LAG)
        def _():
            chip_sum(j - SIB_LAG)

        @pl.when((j >= 5) & (lax.rem(j, 2) == 1))
        def _():
            relay((j - 5) // 2)
        return carry

    lax.fori_loop(0, n_col, down_step, 0)
    for j in range(n_col - SIB_LAG, n_col):
        chip_sum(jnp.int32(j))
    relayed = (n_col - 4) // 2

    def shared_late(i, carry):
        t = A_S1 + i
        wait_pair(t)
        acts[:, cols(EARLY + i, FF_TILE)] = gated(dot(U[own, :], wA[lax.rem(t, DEPTH_A)]))
        relay(relayed + i)
        return carry

    lax.fori_loop(0, n_ff - EARLY, shared_late, 0)
    relayed = relayed + n_ff - EARLY

    def shared_down_step(j, carry):
        b = B_S + j
        waitB(b)
        out_ref[:, cols(j, COL_TILE)] = dot(acts[...], wB[lax.rem(b, DEPTH_B)]).astype(BF)
        issueB(b + DEPTH_B)

        @pl.when((lax.rem(j, 2) == 1) & (relayed + j // 2 < n_col))
        def _():
            relay(relayed + j // 2)
        return carry

    lax.fori_loop(0, n_col, shared_down_step, 0)
    for j in range(relayed + n_col // 2, n_col):
        relay(jnp.int32(j))

    def finish(j, carry):
        last_x(j).wait_recv()
        last_y(j).wait_recv()
        s = cols(j, COL_TILE)
        routed = Pm[chip, :, s] + RX[:, s] + RY[:, s]
        out_ref[:, s] = (xm[:, s].astype(F4) + routed + out_ref[:, s].astype(F4)).astype(BF)

        @pl.when(j >= n_col - SIB_SLOTS)
        def _():
            to_sib(j).wait_send()

        first_leg(j, X).wait_send()
        last_x(j).wait_send()
        last_y(j).wait_send()
        return carry

    lax.fori_loop(0, n_col, finish, 0)


def layer_call(positions, topk_ids, gains, big):
    hidden, w_dq, w_uq = big[0], big[3], big[4]
    tokens, width = hidden.shape
    q_rank = w_dq.shape[1]
    rank = big[1].shape[1]
    ff = big[10].shape[1]
    total = 8 * tokens
    n_col = width // COL_TILE
    n_grp = width // GROUP
    half = ROPE_DIM // 2
    freq = np.zeros((8, LANES), np.float32)
    freq[0, :ROPE_DIM] = np.tile((ROPE_BASE ** (-np.arange(half) / half)).astype(np.float32), 2)
    freq[1, :ROPE_DIM] = np.repeat([-1.0, 1.0], half)
    vmem = pl.BlockSpec(memory_space=pltpu.VMEM)
    smem = pl.BlockSpec(memory_space=pltpu.SMEM)
    hbm = pl.BlockSpec(memory_space=pl.ANY)
    dma = pltpu.SemaphoreType.DMA
    return pl.pallas_call(
        layer_kernel,
        out_shape=(jax.ShapeDtypeStruct((tokens, width), BF), jax.ShapeDtypeStruct((tokens, rank), BF),
                   jax.ShapeDtypeStruct((tokens, ROPE_DIM), BF)),
        in_specs=[smem] + [vmem] * 6 + [hbm] * len(big),
        out_specs=(vmem, vmem, vmem),
        scratch_shapes=[
            pltpu.VMEM((total, width), BF),
            pltpu.VMEM((total, LANES), F4),
            pltpu.VMEM((DEPTH_A, width, 2 * FF_TILE), BF),
            pltpu.VMEM((DEPTH_B, ff, COL_TILE), BF),
            pltpu.VMEM((2, big[5].shape[0], KV_ROWS), BF),
            pltpu.VMEM(big[9].shape, BF),
            pltpu.VMEM(big[2].shape, BF),
            pltpu.VMEM((tokens, big[5].shape[0]), F4),
            pltpu.VMEM((tokens, width), BF),
            pltpu.VMEM((tokens, width), BF),
            pltpu.VMEM((tokens, q_rank), F4),
            pltpu.VMEM((HEADS, tokens, NOPE_DIM), BF),
            pltpu.VMEM((tokens // SUB, HEADS, SUB, rank), F4),
            pltpu.VMEM((tokens // SUB, HEADS, SUB, ROPE_DIM), F4),
            pltpu.VMEM((tokens // SUB, HEADS, SUB, rank), F4),
            pltpu.VMEM((tokens, HEADS * VALUE_DIM), BF),
            pltpu.VMEM((tokens, ff), BF),
            pltpu.VMEM((2, total, ff), BF),
            pltpu.VMEM((4, tokens, width), F4),
            pltpu.VMEM((SIB_SLOTS, 4, tokens, COL_TILE), F4),
            pltpu.VMEM((4, tokens, width), F4),
            pltpu.VMEM((tokens, width), F4),
            pltpu.VMEM((tokens, width), F4),
            pltpu.VMEM((tokens, width), F4),
            dma((2, DEPTH_A)), dma((DEPTH_B,)), dma((2,)), dma((3,)),
        ] + [dma((n_grp,))] * 6 + [dma((4,))] * 2 + [dma((8,))] * 2 + [dma((n_col,))] * 8,
        compiler_params=pltpu.CompilerParams(collective_id=0, has_side_effects=True, vmem_limit_bytes=67043328),
        name='decode_layer',
    )(positions, topk_ids, jnp.asarray(freq), *gains, *big)


def solution(mesh):
    batch = P(('dp', 'ep'))
    whole = P()
    by_expert = P('ep')

    def local_step(hidden, positions, ckv_cache, kpe_cache, topk_ids, attn_gain, w_dq, q_gain, w_uq, w_dkv, kv_gain, w_uk, w_uv, w_out, ffn_gain, w_router, w_gate, w_up, w_down, shared_gate, shared_up, shared_down):
        gains = [attn_gain, q_gain, kv_gain, ffn_gain]
        ckv = ckv_cache.reshape(-1, ckv_cache.shape[2])
        kpe = kpe_cache.reshape(-1, kpe_cache.shape[2])
        big = (hidden, ckv, kpe, w_dq, w_uq, w_dkv.T, w_uk, w_uv, w_out, w_router.T, shared_gate, shared_up, shared_down, w_gate, w_up, w_down)
        return layer_call(positions, topk_ids.T, gains, big)

    in_specs = (batch,) * 5 + (whole,) * 11 + (by_expert,) * 3 + (whole,) * 3
    return jax.shard_map(local_step, mesh=mesh, in_specs=in_specs, out_specs=(batch, batch, batch), check_vma=False)
```

```python
import jax
import jax.numpy as jnp
import numpy as np
from jax import lax
from jax.experimental import pallas as pl
from jax.experimental.pallas import tpu as pltpu
from jax.sharding import PartitionSpec as P

NOPE_DIM = 128
ROPE_DIM = 64
VALUE_DIM = 128
QK_DIM = NOPE_DIM + ROPE_DIM
EPSILON = 1e-6
ROUTE_SCALE = 2.5
ROPE_BASE = 10000.0
CAP_FACTOR = 2
MESH = pl.DeviceIdType.MESH
HEADS = 16
CACHE = 64
FF_TILE = 256
COL_TILE = 512
Q_TILE = 2 * QK_DIM
GROUP = 512
PASS_LAG = 3
KV_TILES = 3
RELAY_LAG = 4
A_AT = 4
DONE_LAG = 6
DEPTH_A = 3
DEPTH_B = 8
LANES = 128
SIB_LAG = 1
SIB_SLOTS = 4
SUB = 8
BF = jnp.bfloat16
F4 = jnp.float32


def layer_kernel(pos_ref, topk, freq, ag, qg, kg, fg,
                 hidden, ckv, kpe, dq, uq, dkv, uk, uv, wo, router, sg, su, sd, wg, wu, wd,
                 out_hbm, cnew_hbm, knew_hbm,
                 topk_ref, freq_ref, ag_ref, qg_ref, kg_ref, fg_ref, out_ref, cnew_ref, knew_ref,
                 U, WT, wA, wB, wR, kp, kvs, hid, xm, cq, QN, QA, QR, CTX, O, acts, part_s, H, ACT, Pm, Ps, R1, RL, RX, RY,
                 semA, semB, semM, as_s, as_r, px_s, px_r, py_s, py_r, pr_s, pr_r, d_s, d_r, w_s, w_r,
                 sib_s, sib_r, rl_s, rl_r, x_s, x_r, y_s, y_r):
    tokens, width = hid.shape
    ff = sg.shape[1]
    rank = uk.shape[0]
    q_rank = cq.shape[1]
    n_ff = ff // FF_TILE
    n_col = width // COL_TILE
    n_grp = width // GROUP
    n_q = uq.shape[1] // Q_TILE
    n_dq = q_rank // COL_TILE
    kv_dim = dkv.shape[0]
    n_kv = (width // COL_TILE + KV_TILES - 1) // KV_TILES
    dp = lax.axis_index('dp')
    me = lax.axis_index('ep')
    core = lax.rem(me, 2)
    chip = me // 2
    cx = lax.rem(chip, 2)
    cy = chip // 2
    kX = cy * 2 + (1 - cx)
    kY = (1 - cy) * 2 + cx
    kD = (1 - cy) * 2 + (1 - cx)
    X = kX * 2 + core
    Y = kY * 2 + core
    sib = chip * 2 + (1 - core)

    def rows(block):
        return pl.ds(pl.multiple_of(block * tokens, tokens), tokens)

    def cols(j, size):
        return pl.ds(pl.multiple_of(j * size, size), size)

    def copy(src, dst, sem):
        return pltpu.make_async_copy(src, dst, sem)

    def rcopy(src, dst, ss, rs, dev):
        return pltpu.make_async_remote_copy(src_ref=src, dst_ref=dst, send_sem=ss, recv_sem=rs,
                                            device_id=(dp, dev), device_id_type=MESH)

    def dot(a, b):
        return jnp.dot(a, b, preferred_element_type=F4)

    def dot_t(a, b):
        return lax.dot_general(a, b, (((1,), (1,)), ((), ())), preferred_element_type=F4)

    A_S0 = n_dq
    A_R = A_S0 + 1
    A_END = A_R + 2 * n_ff

    def issueA(t):
        slot = lax.rem(t, DEPTH_A)

        def pair(left, right):
            copy(left, wA.at[slot, :, 0:FF_TILE], semA.at[0, slot]).start()
            copy(right, wA.at[slot, :, FF_TILE:2 * FF_TILE], semA.at[1, slot]).start()

        @pl.when(t < n_dq)
        def _():
            copy(dq.at[:, cols(t, COL_TILE)], wA.at[slot], semA.at[0, slot]).start()

        @pl.when(t == A_S0)
        def _():
            pair(sg.at[:, cols(me, FF_TILE)], su.at[:, cols(me, FF_TILE)])

        @pl.when((t >= A_R) & (t < A_END))
        def _():
            e = (t - A_R) // n_ff
            n = lax.rem(t - A_R, n_ff)
            pair(wg.at[e, :, cols(n, FF_TILE)], wu.at[e, :, cols(n, FF_TILE)])

    def wait_whole(t):
        slot = lax.rem(t, DEPTH_A)
        copy(dq.at[:, 0:COL_TILE], wA.at[slot], semA.at[0, slot]).wait()

    def wait_pair(t):
        slot = lax.rem(t, DEPTH_A)
        copy(sg.at[:, 0:FF_TILE], wA.at[slot, :, 0:FF_TILE], semA.at[0, slot]).wait()
        copy(su.at[:, 0:FF_TILE], wA.at[slot, :, FF_TILE:2 * FF_TILE], semA.at[1, slot]).wait()

    B_Q = n_kv
    B_UK = B_Q + n_q
    B_CKV = B_UK + 1
    B_UV = B_UK + 2
    B_O = B_UK + 3
    B_D = B_O + n_col
    B_S = B_D + 2 * n_col
    B_END = B_S + n_col

    def issueB(b):
        slot = lax.rem(b, DEPTH_B)

        def blocks(src):
            for q in range(4):
                copy(src.at[:, q * COL_TILE:(q + 1) * COL_TILE], wB.at[slot, q * rank:(q + 1) * rank, :], semB.at[slot]).start()

        @pl.when((b >= B_Q) & (b < B_UK))
        def _():
            copy(uq.at[:, cols(b - B_Q, Q_TILE)], wB.at[slot, 0:q_rank, 0:Q_TILE], semB.at[slot]).start()

        @pl.when(b == B_UK)
        def _():
            blocks(uk)

        @pl.when(b == B_CKV)
        def _():
            copy(ckv, wB.at[slot], semB.at[slot]).start()

        @pl.when(b == B_UV)
        def _():
            blocks(uv)

        @pl.when((b >= B_O) & (b < B_D))
        def _():
            copy(wo.at[:, cols(b - B_O, COL_TILE)], wB.at[slot], semB.at[slot]).start()

        @pl.when((b >= B_D) & (b < B_S))
        def _():
            copy(wd.at[lax.rem(b - B_D, 2), :, cols((b - B_D) // 2, COL_TILE)], wB.at[slot], semB.at[slot]).start()

        @pl.when((b >= B_S) & (b < B_END))
        def _():
            copy(sd.at[:, cols(b - B_S, COL_TILE)], wB.at[slot], semB.at[slot]).start()

    def waitB(b):
        slot = lax.rem(b, DEPTH_B)
        copy(sd.at[:, 0:COL_TILE], wB.at[slot], semB.at[slot]).wait()

    def kv_tiles(b):
        return min(KV_TILES, n_col - b * KV_TILES)

    def issue_kv(b):
        for i in range(kv_tiles(b)):
            first = (b * KV_TILES + i) * COL_TILE
            copy(dkv.at[:, first:first + COL_TILE], wB.at[b, i * kv_dim:(i + 1) * kv_dim, :], semB.at[b]).start()

    def wait_kv(b):
        span = kv_tiles(b) * kv_dim
        copy(sd.at[0:span, 0:COL_TILE], wB.at[b, 0:span, :], semB.at[b]).wait()

    small = [copy(hidden, hid, semM.at[0]), copy(kpe, kp, semM.at[1]), copy(router, wR, semM.at[2]), copy(topk, topk_ref, semM.at[3]),
             copy(freq, freq_ref, semM.at[4]), copy(ag, ag_ref, semM.at[5]), copy(qg, qg_ref, semM.at[6]), copy(kg, kg_ref, semM.at[7]), copy(fg, fg_ref, semM.at[8])]
    small[0].start()
    small[5].start()
    small[4].start()
    for b in range(n_kv):
        issue_kv(b)
    issueA(jnp.int32(0))
    issueA(jnp.int32(1))
    for i in (6, 7, 8, 3, 1, 2):
        small[i].start()

    barrier = pltpu.get_barrier_semaphore()
    for k in range(1, 8):
        pl.semaphore_signal(barrier, inc=1, device_id=(dp, lax.rem(me + k, 8)), device_id_type=MESH)

    def rotate(v):
        other = jnp.concatenate([v[:, ROPE_DIM // 2:], v[:, :ROPE_DIM // 2]], axis=1)
        return v * cosine + other * sine

    def gain(ref):
        return ref[...].astype(F4).reshape(1, -1)

    def rms(v, gain):
        scale = lax.rsqrt(jnp.mean(v * v, axis=-1, keepdims=True) + EPSILON)
        return v * scale * gain

    small[0].wait()
    small[5].wait()
    own = rows(chip)
    U[own, :] = rms(hid[...].astype(F4), gain(ag_ref)).astype(BF)

    kvs[...] = jnp.zeros_like(kvs)
    for b in range(n_kv):
        wait_kv(b)
        part = kvs[...]
        for i in range(kv_tiles(b)):
            first = (b * KV_TILES + i) * COL_TILE
            part = part + dot_t(U[own, first:first + COL_TILE], wB[b, i * kv_dim:(i + 1) * kv_dim, :])
        kvs[...] = part
        if b == 0:
            issueA(jnp.int32(2))
    for b in range(n_kv, n_kv + DEPTH_B):
        issueB(jnp.int32(b))
    for t in range(n_dq):
        wait_whole(t)
        cq[:, t * COL_TILE:(t + 1) * COL_TILE] = dot(U[own, :], wA[t])
    small[6].wait()
    small[7].wait()
    small[4].wait()

    row_id = lax.broadcasted_iota(jnp.int32, (tokens, ROPE_DIM), 0)
    posv = jnp.zeros((tokens, ROPE_DIM), jnp.int32)
    for t in range(tokens):
        posv = jnp.where(row_id == t, pos_ref[t], posv)
    angle = posv.astype(F4) * freq_ref[0:1, 0:ROPE_DIM]
    cosine = jnp.cos(angle)
    sine = jnp.sin(angle) * freq_ref[1:2, 0:ROPE_DIM]
    c_q = rms(cq[...], gain(qg_ref)).astype(BF)
    cq[...] = c_q.astype(F4)

    def put(ref, h, val):
        for g in range(tokens // SUB):
            ref[g, h] = val[g * SUB:(g + 1) * SUB]

    def uq_step(i, carry):
        parts = []
        for k in range(2):
            b = B_Q + 2 * i + k
            slot = lax.rem(b, DEPTH_B)
            copy(uq.at[:, 0:Q_TILE], wB.at[slot, 0:q_rank, 0:Q_TILE], semB.at[slot]).wait()
        for k in range(2):
            b = B_Q + 2 * i + k
            parts.append(dot(cq[...].astype(BF), wB[lax.rem(b, DEPTH_B), 0:q_rank, 0:Q_TILE]).astype(BF).astype(F4))
        for k in range(2):
            issueB(B_Q + 2 * i + k + DEPTH_B)
        for h in range(4):
            q2 = parts[h // 2]
            base = (h % 2) * QK_DIM
            QN[4 * i + h] = q2[:, base:base + NOPE_DIM].astype(BF)
            put(QR, 4 * i + h, rotate(q2[:, base + NOPE_DIM:base + QK_DIM]).astype(BF).astype(F4))
        return carry

    lax.fori_loop(0, n_q // 2, uq_step, 0)
    issueA(jnp.int32(n_dq))

    cnew_ref[...] = rms(kvs[:, 0:rank], gain(kg_ref)).astype(BF)
    knew_ref[...] = rotate(kvs[:, rank:rank + ROPE_DIM]).astype(BF)
    c_out = copy(cnew_ref, cnew_hbm, semM.at[9])
    k_out = copy(knew_ref, knew_hbm, semM.at[10])
    c_out.start()
    k_out.start()

    waitB(B_UK)
    slot_uk = B_UK % DEPTH_B

    for h in range(HEADS):
        w_h = wB[slot_uk, (h // 4) * rank:(h // 4 + 1) * rank, (h % 4) * NOPE_DIM:(h % 4 + 1) * NOPE_DIM]
        put(QA, h, dot_t(QN[h], w_h).astype(BF).astype(F4))
    issueB(jnp.int32(B_UK + DEPTH_B))

    waitB(B_CKV)
    slot_ckv = B_CKV % DEPTH_B
    small[1].wait()
    span = SUB * CACHE
    scale = QK_DIM ** -0.5
    lane = lax.broadcasted_iota(jnp.int32, (SUB, span), 1)
    tok = lax.broadcasted_iota(jnp.int32, (SUB, span), 0)
    for g in range(tokens // SUB):
        keys = wB[slot_ckv, g * span:(g + 1) * span, :]
        qa = QA[g]
        qr = QR[g]
        cn = cnew_ref[g * SUB:(g + 1) * SUB, :].astype(F4)
        kn = knew_ref[g * SUB:(g + 1) * SUB, :].astype(F4)
        s = dot_t(qa.reshape(HEADS * SUB, rank).astype(BF), keys)
        s = s + dot_t(qr.reshape(HEADS * SUB, ROPE_DIM).astype(BF), kp[g * span:(g + 1) * span, :])
        s = s.reshape(HEADS, SUB, span) * scale
        limit = posv[g * SUB:(g + 1) * SUB, 0:1]
        valid = (lane >= tok * CACHE) & (lane < tok * CACHE + limit)
        s = jnp.where(valid[None], s, -1e30)
        s_self = (jnp.sum(qa * cn[None], axis=2, keepdims=True) + jnp.sum(qr * kn[None], axis=2, keepdims=True)) * scale
        peak = jnp.maximum(jnp.max(s, axis=2, keepdims=True), s_self)
        e = jnp.where(valid[None], jnp.exp(s - peak), 0.0)
        e_self = jnp.exp(s_self - peak)
        denom = jnp.sum(e, axis=2, keepdims=True) + e_self
        p = (e / denom).astype(BF)
        p_self = (e_self / denom).astype(BF).astype(F4)
        ctx = dot(p.reshape(HEADS * SUB, span), keys).reshape(HEADS, SUB, rank) + p_self * cn[None]
        CTX[g] = ctx.astype(BF).astype(F4)
    issueB(jnp.int32(B_CKV + DEPTH_B))

    waitB(B_UV)
    slot_uv = B_UV % DEPTH_B
    for h in range(HEADS):
        w_h = wB[slot_uv, (h // 4) * rank:(h // 4 + 1) * rank, (h % 4) * VALUE_DIM:(h % 4 + 1) * VALUE_DIM]
        O[:, h * VALUE_DIM:(h + 1) * VALUE_DIM] = dot(CTX[:, h].reshape(tokens, rank).astype(BF), w_h).astype(BF)
    issueB(jnp.int32(B_UV + DEPTH_B))

    pl.semaphore_wait(barrier, 7)

    def grp_x(p, block):
        return rcopy(xm.at[:, cols(p, GROUP)], U.at[rows(block), cols(p, GROUP)], px_s.at[p], px_r.at[p], X)

    def grp_y(p, block):
        return rcopy(xm.at[:, cols(p, GROUP)], U.at[rows(block), cols(p, GROUP)], py_s.at[p], py_r.at[p], Y)

    def pass_y(p, block):
        return rcopy(U.at[rows(kX), cols(p, GROUP)], U.at[rows(block), cols(p, GROUP)], pr_s.at[p], pr_r.at[p], Y)

    def pass_x(p, block):
        return rcopy(U.at[rows(kY), cols(p, GROUP)], U.at[rows(block), cols(p, GROUP)], pr_s.at[p], pr_r.at[p], X)

    def forward(p):
        odd = lax.rem(p, 2)

        @pl.when(odd == 0)
        def _():
            grp_x(p, kX).wait_recv()
            pass_y(p, kX).start()

        @pl.when(odd == 1)
        def _():
            grp_y(p, kY).wait_recv()
            pass_x(p, kY).start()

    def send_rest(first, last):
        for p in range(first, last):
            if p % 2 == 0:
                grp_y(p, chip).start()
            else:
                grp_x(p, chip).start()

    def out_step(i, carry):
        b = B_O + 2 * i
        waitB(b)
        waitB(b + 1)
        both = [dot(O[...], wB[lax.rem(b + k, DEPTH_B)]) for k in range(2)]
        for k in range(2):
            s = cols(2 * i + k, COL_TILE)
            xm[:, s] = (hid[:, s].astype(F4) + both[k]).astype(BF)
        grp_x(2 * i, chip).start()
        grp_y(2 * i + 1, chip).start()
        issueB(b + DEPTH_B)
        issueB(b + 1 + DEPTH_B)

        @pl.when(i < PASS_LAG)
        def _():
            grp_y(2 * i, chip).start()
            grp_x(2 * i + 1, chip).start()

        @pl.when(i >= PASS_LAG)
        def _():
            forward(2 * (i - PASS_LAG))
            forward(2 * (i - PASS_LAG) + 1)

        @pl.when((i >= A_AT) & (i < A_AT + DEPTH_A - 1))
        def _():
            issueA(i - A_AT + n_dq + 1)
        return carry

    lax.fori_loop(0, n_col // 2, out_step, 0)
    send_rest(2 * PASS_LAG, 2 * PASS_LAG + 2)

    small[8].wait()
    u_own = rms(xm[...].astype(F4), gain(fg_ref)).astype(BF)
    U[own, :] = u_own
    toS = rcopy(U.at[own, :], U.at[rows(4 + chip), :], d_s.at[0], d_r.at[0], sib)
    toS.start()
    small[2].wait()
    small[3].wait()
    experts = router.shape[0]
    capacity = (CAP_FACTOR * tokens * topk_ref.shape[0] + experts - 1) // experts
    gates = jax.nn.sigmoid(dot_t(U[own, :], wR[...]))
    eid = lax.broadcasted_iota(jnp.int32, (experts, tokens), 0)
    picks = jnp.zeros((experts, tokens), F4)
    for k in range(topk_ref.shape[0]):
        picks = picks + jnp.where(topk_ref[k:k + 1, :] == eid, 1.0, 0.0)
    picks = picks.astype(BF)
    here = lax.broadcasted_iota(jnp.int32, (tokens, tokens), 0)
    there = lax.broadcasted_iota(jnp.int32, (tokens, tokens), 1)
    hits = dot_t(jnp.where(here == there, 1.0, 0.0).astype(BF), picks)
    before = dot_t(jnp.where(here > there, 1.0, 0.0).astype(BF), picks)
    total = jnp.sum(hits * gates, axis=1, keepdims=True)
    table = jnp.where(before < capacity, hits, 0.0) * (ROUTE_SCALE * gates / total)
    WT[own, 0:experts] = table

    WT[own, experts:LANES] = jnp.zeros((tokens, LANES - experts), F4)
    D = kD * 2 + core
    mates = ((1, kX, X), (2, kY, Y), (3, kD, D))

    def table_to(i, dev):
        return rcopy(WT.at[own, :], WT.at[own, :], w_s.at[i], w_r.at[i], dev)

    def table_from(i, k, dev):
        return rcopy(WT.at[rows(k), :], WT.at[rows(k), :], w_s.at[i], w_r.at[i], dev)

    def tables_to_twin():
        return rcopy(WT.at[0:4 * tokens, :], WT.at[4 * tokens:8 * tokens, :], w_s.at[0], w_r.at[0], sib)

    for i, _, dev in mates:
        table_to(i, dev).start()

    def gated(both):
        g = both[:, 0:FF_TILE]
        return (g * jax.nn.sigmoid(g) * both[:, FF_TILE:2 * FF_TILE]).astype(BF)

    def to_twin(i, k):
        return rcopy(U.at[rows(k), :], U.at[rows(4 + k), :], d_s.at[i], d_r.at[i], sib)

    def normalise(block):
        r = rows(block)
        U[r, :] = rms(U[r, :].astype(F4), gain(fg_ref)).astype(BF)

    for p in range(n_grp - 2 * PASS_LAG, n_grp, 2):
        forward(jnp.int32(p))
        forward(jnp.int32(p + 1))
        if p > n_grp - 2 * PASS_LAG:
            q = p - n_grp + 4 * PASS_LAG
            send_rest(min(q, n_grp), min(q + 2, n_grp))
    send_rest(4 * PASS_LAG, n_grp)
    for p in range(1, n_grp, 2):
        grp_x(p, kX).wait_recv()
        pass_x(p, kY).wait_send()
    for p in range(0, n_grp, 2):
        pass_y(p, kX).wait_send()
    normalise(kX)
    to_twin(1, kX).start()
    for p in range(0, n_grp, 2):
        grp_y(p, kY).wait_recv()
    normalise(kY)
    to_twin(2, kY).start()
    for p in range(n_grp):
        if p % 2 == 0:
            pass_y(p, kD).wait_recv()
        else:
            pass_x(p, kD).wait_recv()
    normalise(kD)
    to_twin(3, kD).start()
    wait_pair(A_S0)
    part_s[0:4 * tokens, :] = gated(dot(U[0:4 * tokens, :], wA[A_S0 % DEPTH_A]))
    for i, k, dev in mates:
        table_from(i, k, dev).wait_recv()
    tables_to_twin().start()
    rcopy(U.at[own, :], U.at[rows(4 + chip), :], d_s.at[0], d_r.at[0], sib).wait_recv()
    for i, k in ((1, kX), (2, kY), (3, kD)):
        rcopy(U.at[rows(k), :], U.at[rows(4 + k), :], d_s.at[i], d_r.at[i], sib).wait_recv()
    part_s[4 * tokens:8 * tokens, :] = gated(dot(U[4 * tokens:8 * tokens, :], wA[A_S0 % DEPTH_A]))
    issueA(jnp.int32(A_S0 + DEPTH_A))
    toS.wait_send()
    for i, k in ((1, kX), (2, kY), (3, kD)):
        to_twin(i, k).wait_send()
    for p in range(n_grp):
        grp_x(p, chip).wait_send()
        grp_y(p, chip).wait_send()

    def act_to(k):
        dev = lax.rem(me + k, 8)
        block = dev // 2 + 4 * lax.rem(core + dev, 2)
        return rcopy(part_s.at[rows(block), :], acts.at[:, cols(me, FF_TILE)], as_s.at[k], as_r.at[k], dev)

    def act_from(k):
        dev = lax.rem(me + 8 - k, 8)
        return rcopy(part_s.at[own, :], acts.at[:, cols(dev, FF_TILE)], as_s.at[k], as_r.at[k], dev)

    for k in range(1, 8):
        act_to(k).start()
    acts[:, cols(me, FF_TILE)] = part_s[own, :]

    def routed_up_step(i, carry):
        t = A_R + i
        wait_pair(t)
        last = i - 1
        ACT[last // n_ff, :, cols(lax.rem(last, n_ff), FF_TILE)] = gated(H[lax.rem(last, 2)])
        H[lax.rem(i, 2)] = dot(U[...], wA[lax.rem(t, DEPTH_A)])
        issueA(t + DEPTH_A)
        return carry

    wait_pair(A_R)
    H[0] = dot(U[...], wA[A_R % DEPTH_A])
    issueA(jnp.int32(A_R + DEPTH_A))
    lax.fori_loop(1, 2 * n_ff, routed_up_step, 0)
    ACT[1, :, ff - FF_TILE:ff] = gated(H[(2 * n_ff - 1) % 2])

    for i, _, dev in mates:
        table_to(i, dev).wait_send()
    tables_to_twin().wait()

    lane_id = lax.broadcasted_iota(jnp.int32, WT.shape, 1)
    w0 = jnp.sum(jnp.where(lane_id == 2 * me, WT[...], 0.0), axis=1, keepdims=True)
    w1 = jnp.sum(jnp.where(lane_id == 2 * me + 1, WT[...], 0.0), axis=1, keepdims=True)

    def to_sib(j):
        return rcopy(Ps.at[lax.rem(j, SIB_SLOTS)], R1.at[:, :, cols(j, COL_TILE)], sib_s.at[j], sib_r.at[j], sib)

    def first_leg(j, dev):
        return rcopy(Pm.at[kD, :, cols(j, COL_TILE)], RL.at[:, cols(j, COL_TILE)], rl_s.at[j], rl_r.at[j], dev)

    def last_x(j):
        return rcopy(Pm.at[kX, :, cols(j, COL_TILE)], RX.at[:, cols(j, COL_TILE)], x_s.at[j], x_r.at[j], X)

    def last_y(j):
        return rcopy(Pm.at[kY, :, cols(j, COL_TILE)], RY.at[:, cols(j, COL_TILE)], y_s.at[j], y_r.at[j], Y)

    def chip_sum(j):
        to_sib(j).wait_recv()
        Pm[:, :, cols(j, COL_TILE)] = Pm[:, :, cols(j, COL_TILE)] + R1[:, :, cols(j, COL_TILE)]
        odd = lax.rem(j, 2)

        @pl.when(odd == 0)
        def _():
            first_leg(j, X).start()

            @pl.when(j < RELAY_LAG)
            def _():
                last_x(j).start()

        @pl.when(odd == 1)
        def _():
            first_leg(j, Y).start()

            @pl.when(j < RELAY_LAG)
            def _():
                last_y(j).start()

    def relay(j):
        odd = lax.rem(j, 2)

        @pl.when(odd == 0)
        def _():
            first_leg(j, X).wait_recv()
            Pm[kY, :, cols(j, COL_TILE)] = Pm[kY, :, cols(j, COL_TILE)] + RL[:, cols(j, COL_TILE)]
            last_y(j).start()

        @pl.when(odd == 1)
        def _():
            first_leg(j, Y).wait_recv()
            Pm[kX, :, cols(j, COL_TILE)] = Pm[kX, :, cols(j, COL_TILE)] + RL[:, cols(j, COL_TILE)]
            last_x(j).start()

    def down_step(j, carry):
        b = B_D + 2 * j
        waitB(b)
        waitB(b + 1)
        e0 = dot(ACT[0], wB[lax.rem(b, DEPTH_B)]).astype(BF)
        e1 = dot(ACT[1], wB[lax.rem(b + 1, DEPTH_B)]).astype(BF)

        @pl.when(j >= SIB_SLOTS)
        def _():
            to_sib(j - SIB_SLOTS).wait_send()

        part = w0 * e0.astype(F4) + w1 * e1.astype(F4)
        Pm[:, :, cols(j, COL_TILE)] = part[0:4 * tokens].reshape(4, tokens, COL_TILE)
        Ps[lax.rem(j, SIB_SLOTS)] = part[4 * tokens:8 * tokens].reshape(4, tokens, COL_TILE)
        to_sib(j).start()
        issueB(b + DEPTH_B)
        issueB(b + 1 + DEPTH_B)

        @pl.when(j >= SIB_LAG)
        def _():
            chip_sum(j - SIB_LAG)

        @pl.when(j >= RELAY_LAG)
        def _():
            relay(j - RELAY_LAG)
        return carry

    lax.fori_loop(0, n_col, down_step, 0)
    for j in range(n_col - SIB_LAG, n_col):
        chip_sum(jnp.int32(j))
    for j in range(RELAY_LAG, n_col):
        if j % 2 == 0:
            last_x(jnp.int32(j)).start()
        else:
            last_y(jnp.int32(j)).start()
    relayed = n_col - RELAY_LAG

    for k in range(1, 8):
        act_from(k).wait_recv()
        act_to(k).wait_send()

    def result(j):
        return copy(out_ref.at[:, cols(j, COL_TILE)], out_hbm.at[:, cols(j, COL_TILE)], semM.at[11])

    def finish(j, carry):
        last_x(j).wait_recv()
        last_y(j).wait_recv()
        s = cols(j, COL_TILE)
        routed = Pm[chip, :, s] + RX[:, s] + RY[:, s]
        out_ref[:, s] = (xm[:, s].astype(F4) + routed + out_ref[:, s].astype(F4)).astype(BF)
        result(j).start()
        return carry

    def shared_down_step(j, carry):
        b = B_S + j
        waitB(b)
        out_ref[:, cols(j, COL_TILE)] = dot(acts[...], wB[lax.rem(b, DEPTH_B)]).astype(BF)
        issueB(b + DEPTH_B)

        @pl.when(relayed + j < n_col)
        def _():
            relay(relayed + j)

        @pl.when(j >= DONE_LAG)
        def _():
            finish(j - DONE_LAG, 0)
        return carry

    lax.fori_loop(0, n_col, shared_down_step, 0)
    lax.fori_loop(n_col - DONE_LAG, n_col, finish, 0)
    for j in range(n_col):
        if j >= n_col - SIB_SLOTS:
            to_sib(j).wait_send()
        first_leg(j, X).wait_send()
        last_x(j).wait_send()
        last_y(j).wait_send()
    c_out.wait()
    k_out.wait()
    copy(out_ref, out_hbm, semM.at[11]).wait()


def hand_on(a, b, c, oa, ob, oc, va, vb, vc, sems):
    pairs = ((a, va, oa), (b, vb, ob), (c, vc, oc))
    for i, (src, mid, _) in enumerate(pairs):
        pltpu.make_async_copy(src, mid, sems.at[0, i]).start()
    for i, (src, mid, dst) in enumerate(pairs):
        pltpu.make_async_copy(src, mid, sems.at[0, i]).wait()
        pltpu.make_async_copy(mid, dst, sems.at[1, i]).start()
    for i, (_, mid, dst) in enumerate(pairs):
        pltpu.make_async_copy(mid, dst, sems.at[1, i]).wait()


def layer_call(positions, topk_ids, gains, big):
    hidden, w_dq, w_uq = big[0], big[3], big[4]
    tokens, width = hidden.shape
    q_rank = w_dq.shape[1]
    rank = big[1].shape[1]
    ff = big[10].shape[1]
    total = 8 * tokens
    n_col = width // COL_TILE
    n_grp = width // GROUP
    half = ROPE_DIM // 2
    freq = np.zeros((8, LANES), np.float32)
    freq[0, :ROPE_DIM] = np.tile((ROPE_BASE ** (-np.arange(half) / half)).astype(np.float32), 2)
    freq[1, :ROPE_DIM] = np.repeat([-1.0, 1.0], half)
    smem = pl.BlockSpec(memory_space=pltpu.SMEM)
    hbm = pl.BlockSpec(memory_space=pl.ANY)
    dma = pltpu.SemaphoreType.DMA
    shapes = [(tokens, width), (tokens, rank), (tokens, ROPE_DIM)]
    outs = tuple(jax.ShapeDtypeStruct(shape, BF) for shape in shapes)
    results = pl.pallas_call(
        layer_kernel,
        out_shape=outs,
        in_specs=[smem] + [hbm] * (6 + len(big)),
        out_specs=(hbm, hbm, hbm),
        scratch_shapes=[pltpu.VMEM(topk_ids.shape, jnp.int32), pltpu.VMEM(freq.shape, F4)]
        + [pltpu.VMEM(g.shape, BF) for g in gains] + [pltpu.VMEM(shape, BF) for shape in shapes] + [
            pltpu.VMEM((total, width), BF),
            pltpu.VMEM((total, LANES), F4),
            pltpu.VMEM((DEPTH_A, width, 2 * FF_TILE), BF),
            pltpu.VMEM((DEPTH_B, ff, COL_TILE), BF),
            pltpu.VMEM(big[9].shape, BF),
            pltpu.VMEM(big[2].shape, BF),
            pltpu.VMEM((tokens, big[5].shape[0]), F4),
            pltpu.VMEM((tokens, width), BF),
            pltpu.VMEM((tokens, width), BF),
            pltpu.VMEM((tokens, q_rank), F4),
            pltpu.VMEM((HEADS, tokens, NOPE_DIM), BF),
            pltpu.VMEM((tokens // SUB, HEADS, SUB, rank), F4),
            pltpu.VMEM((tokens // SUB, HEADS, SUB, ROPE_DIM), F4),
            pltpu.VMEM((tokens // SUB, HEADS, SUB, rank), F4),
            pltpu.VMEM((tokens, HEADS * VALUE_DIM), BF),
            pltpu.VMEM((tokens, ff), BF),
            pltpu.VMEM((total, FF_TILE), BF),
            pltpu.VMEM((2, total, 2 * FF_TILE), F4),
            pltpu.VMEM((2, total, ff), BF),
            pltpu.VMEM((4, tokens, width), F4),
            pltpu.VMEM((SIB_SLOTS, 4, tokens, COL_TILE), F4),
            pltpu.VMEM((4, tokens, width), F4),
            pltpu.VMEM((tokens, width), F4),
            pltpu.VMEM((tokens, width), F4),
            pltpu.VMEM((tokens, width), F4),
            dma((2, DEPTH_A)), dma((DEPTH_B,)), dma((12,)), dma((8,)), dma((8,)),
        ] + [dma((n_grp,))] * 6 + [dma((4,))] * 4 + [dma((n_col,))] * 8,
        compiler_params=pltpu.CompilerParams(collective_id=0, has_side_effects=True, vmem_limit_bytes=67043328),
        name='decode_layer',
    )(positions, topk_ids, jnp.asarray(freq), *gains, *big)
    return pl.pallas_call(
        hand_on,
        out_shape=outs,
        in_specs=[hbm] * 3,
        out_specs=(hbm, hbm, hbm),
        scratch_shapes=[pltpu.VMEM(shape, BF) for shape in shapes] + [dma((2, 3))],
        name='hand_on',
    )(*results)


def solution(mesh):
    batch = P(('dp', 'ep'))
    whole = P()
    by_expert = P('ep')

    def local_step(hidden, positions, ckv_cache, kpe_cache, topk_ids, attn_gain, w_dq, q_gain, w_uq, w_dkv, kv_gain, w_uk, w_uv, w_out, ffn_gain, w_router, w_gate, w_up, w_down, shared_gate, shared_up, shared_down):
        gains = [attn_gain, q_gain, kv_gain, ffn_gain]
        ckv = ckv_cache.reshape(-1, ckv_cache.shape[2])
        kpe = kpe_cache.reshape(-1, kpe_cache.shape[2])
        big = (hidden, ckv, kpe, w_dq, w_uq, w_dkv.T, w_uk, w_uv, w_out, w_router.T, shared_gate, shared_up, shared_down, w_gate, w_up, w_down)
        return layer_call(positions, topk_ids.T, gains, big)

    in_specs = (batch,) * 5 + (whole,) * 11 + (by_expert,) * 3 + (whole,) * 3
    return jax.shard_map(local_step, mesh=mesh, in_specs=in_specs, out_specs=(batch, batch, batch), check_vma=False)
```

```python
import jax
import jax.numpy as jnp
import numpy as np
from jax import lax
from jax.experimental import pallas as pl
from jax.experimental.pallas import tpu as pltpu
from jax.sharding import PartitionSpec as P

NOPE_DIM = 128
ROPE_DIM = 64
VALUE_DIM = 128
QK_DIM = NOPE_DIM + ROPE_DIM
EPSILON = 1e-6
ROUTE_SCALE = 2.5
ROPE_BASE = 10000.0
CAP_FACTOR = 2
MESH = pl.DeviceIdType.MESH
HEADS = 16
CACHE = 64
FF_TILE = 256
COL_TILE = 512
Q_TILE = 2 * QK_DIM
GROUP = 512
PASS_LAG = 3
KV_TILES = 3
RELAY_LAG = 4
A_AT = 4
DONE_LAG = 6
DEPTH_A = 3
DEPTH_B = 8
LANES = 128
SIB_LAG = 1
SIB_SLOTS = 4
SUB = 8
BF = jnp.bfloat16
F4 = jnp.float32


def layer_kernel(pos_ref, topk, freq, ag, qg, kg, fg,
                 hidden, ckv, kpe, dq, uq, dkv, uk, uv, wo, router, sg, su, sd, wg, wu, wd,
                 out_hbm, cnew_hbm, knew_hbm,
                 topk_ref, freq_ref, ag_ref, qg_ref, kg_ref, fg_ref, out_ref, cnew_ref, knew_ref,
                 U, WT, wA, wB, wR, kp, kvs, hid, xm, cq, QN, QA, QR, O, acts, part_s, H, ACT, Pm, Ps, R1, RL, RX, RY,
                 semA, semB, semM, as_s, as_r, px_s, px_r, py_s, py_r, pr_s, pr_r, d_s, d_r, w_s, w_r,
                 sib_s, sib_r, rl_s, rl_r, x_s, x_r, y_s, y_r):
    tokens, width = hid.shape
    ff = sg.shape[1]
    rank = uk.shape[0]
    q_rank = cq.shape[1]
    n_ff = ff // FF_TILE
    n_col = width // COL_TILE
    n_grp = width // GROUP
    n_q = uq.shape[1] // Q_TILE
    n_dq = q_rank // COL_TILE
    kv_dim = dkv.shape[0]
    n_kv = (width // COL_TILE + KV_TILES - 1) // KV_TILES
    dp = lax.axis_index('dp')
    me = lax.axis_index('ep')
    core = lax.rem(me, 2)
    chip = me // 2
    cx = lax.rem(chip, 2)
    cy = chip // 2
    kX = cy * 2 + (1 - cx)
    kY = (1 - cy) * 2 + cx
    kD = (1 - cy) * 2 + (1 - cx)
    X = kX * 2 + core
    Y = kY * 2 + core
    sib = chip * 2 + (1 - core)

    def rows(block):
        return pl.ds(pl.multiple_of(block * tokens, tokens), tokens)

    def cols(j, size):
        return pl.ds(pl.multiple_of(j * size, size), size)

    def copy(src, dst, sem):
        return pltpu.make_async_copy(src, dst, sem)

    def rcopy(src, dst, ss, rs, dev):
        return pltpu.make_async_remote_copy(src_ref=src, dst_ref=dst, send_sem=ss, recv_sem=rs,
                                            device_id=(dp, dev), device_id_type=MESH)

    def dot(a, b):
        return jnp.dot(a, b, preferred_element_type=F4)

    def dot_t(a, b):
        return lax.dot_general(a, b, (((1,), (1,)), ((), ())), preferred_element_type=F4)

    A_S0 = n_dq
    A_R = A_S0 + 1
    A_END = A_R + 2 * n_ff

    def issueA(t):
        slot = lax.rem(t, DEPTH_A)

        def pair(left, right):
            copy(left, wA.at[slot, :, 0:FF_TILE], semA.at[0, slot]).start()
            copy(right, wA.at[slot, :, FF_TILE:2 * FF_TILE], semA.at[1, slot]).start()

        @pl.when(t < n_dq)
        def _():
            copy(dq.at[:, cols(t, COL_TILE)], wA.at[slot], semA.at[0, slot]).start()

        @pl.when(t == A_S0)
        def _():
            pair(sg.at[:, cols(me, FF_TILE)], su.at[:, cols(me, FF_TILE)])

        @pl.when((t >= A_R) & (t < A_END))
        def _():
            e = (t - A_R) // n_ff
            n = lax.rem(t - A_R, n_ff)
            pair(wg.at[e, :, cols(n, FF_TILE)], wu.at[e, :, cols(n, FF_TILE)])

    def wait_whole(t):
        slot = lax.rem(t, DEPTH_A)
        copy(dq.at[:, 0:COL_TILE], wA.at[slot], semA.at[0, slot]).wait()

    def wait_pair(t):
        slot = lax.rem(t, DEPTH_A)
        copy(sg.at[:, 0:FF_TILE], wA.at[slot, :, 0:FF_TILE], semA.at[0, slot]).wait()
        copy(su.at[:, 0:FF_TILE], wA.at[slot, :, FF_TILE:2 * FF_TILE], semA.at[1, slot]).wait()

    B_Q = n_kv
    B_UK = B_Q + n_q
    B_CKV = B_UK + 1
    B_UV = B_UK + 2
    B_O = B_UK + 3
    B_D = B_O + n_col
    B_S = B_D + 2 * n_col
    B_END = B_S + n_col

    def issueB(b):
        slot = lax.rem(b, DEPTH_B)

        def blocks(src):
            for q in range(4):
                copy(src.at[:, q * COL_TILE:(q + 1) * COL_TILE], wB.at[slot, q * rank:(q + 1) * rank, :], semB.at[slot]).start()

        @pl.when((b >= B_Q) & (b < B_UK))
        def _():
            copy(uq.at[:, cols(b - B_Q, Q_TILE)], wB.at[slot, 0:q_rank, 0:Q_TILE], semB.at[slot]).start()

        @pl.when(b == B_UK)
        def _():
            blocks(uk)

        @pl.when(b == B_CKV)
        def _():
            copy(ckv, wB.at[slot], semB.at[slot]).start()

        @pl.when(b == B_UV)
        def _():
            blocks(uv)

        @pl.when((b >= B_O) & (b < B_D))
        def _():
            copy(wo.at[:, cols(b - B_O, COL_TILE)], wB.at[slot], semB.at[slot]).start()

        @pl.when((b >= B_D) & (b < B_S))
        def _():
            copy(wd.at[lax.rem(b - B_D, 2), :, cols((b - B_D) // 2, COL_TILE)], wB.at[slot], semB.at[slot]).start()

        @pl.when((b >= B_S) & (b < B_END))
        def _():
            copy(sd.at[:, cols(b - B_S, COL_TILE)], wB.at[slot], semB.at[slot]).start()

    def waitB(b):
        slot = lax.rem(b, DEPTH_B)
        copy(sd.at[:, 0:COL_TILE], wB.at[slot], semB.at[slot]).wait()

    def kv_tiles(b):
        return min(KV_TILES, n_col - b * KV_TILES)

    def issue_kv(b):
        for i in range(kv_tiles(b)):
            first = (b * KV_TILES + i) * COL_TILE
            copy(dkv.at[:, first:first + COL_TILE], wB.at[b, i * kv_dim:(i + 1) * kv_dim, :], semB.at[b]).start()

    def wait_kv(b):
        span = kv_tiles(b) * kv_dim
        copy(sd.at[0:span, 0:COL_TILE], wB.at[b, 0:span, :], semB.at[b]).wait()

    small = [copy(hidden, hid, semM.at[0]), copy(kpe, kp, semM.at[1]), copy(router, wR, semM.at[2]), copy(topk, topk_ref, semM.at[3]),
             copy(freq, freq_ref, semM.at[4]), copy(ag, ag_ref, semM.at[5]), copy(qg, qg_ref, semM.at[6]), copy(kg, kg_ref, semM.at[7]), copy(fg, fg_ref, semM.at[8])]
    small[0].start()
    small[5].start()
    small[4].start()
    for b in range(n_kv):
        issue_kv(b)
    issueA(jnp.int32(0))
    issueA(jnp.int32(1))
    for i in (6, 7, 8, 3, 1, 2):
        small[i].start()

    barrier = pltpu.get_barrier_semaphore()
    for k in range(1, 8):
        pl.semaphore_signal(barrier, inc=1, device_id=(dp, lax.rem(me + k, 8)), device_id_type=MESH)

    def rotate(v):
        other = jnp.concatenate([v[:, ROPE_DIM // 2:], v[:, :ROPE_DIM // 2]], axis=1)
        return v * cosine + other * sine

    def gain(ref):
        return ref[...].astype(F4).reshape(1, -1)

    def rms(v, gain):
        scale = lax.rsqrt(jnp.mean(v * v, axis=-1, keepdims=True) + EPSILON)
        return v * scale * gain

    small[0].wait()
    small[5].wait()
    own = rows(chip)
    U[own, :] = rms(hid[...].astype(F4), gain(ag_ref)).astype(BF)

    kvs[...] = jnp.zeros_like(kvs)
    for b in range(n_kv):
        wait_kv(b)
        part = kvs[...]
        for i in range(kv_tiles(b)):
            first = (b * KV_TILES + i) * COL_TILE
            part = part + dot_t(U[own, first:first + COL_TILE], wB[b, i * kv_dim:(i + 1) * kv_dim, :])
        kvs[...] = part
        if b == 0:
            issueA(jnp.int32(2))
    for b in range(n_kv, n_kv + DEPTH_B):
        issueB(jnp.int32(b))
    for t in range(n_dq):
        wait_whole(t)
        cq[:, t * COL_TILE:(t + 1) * COL_TILE] = dot(U[own, :], wA[t])
    small[6].wait()
    small[7].wait()
    small[4].wait()

    row_id = lax.broadcasted_iota(jnp.int32, (tokens, ROPE_DIM), 0)
    posv = jnp.zeros((tokens, ROPE_DIM), jnp.int32)
    for t in range(tokens):
        posv = jnp.where(row_id == t, pos_ref[t], posv)
    angle = posv.astype(F4) * freq_ref[0:1, 0:ROPE_DIM]
    cosine = jnp.cos(angle)
    sine = jnp.sin(angle) * freq_ref[1:2, 0:ROPE_DIM]
    c_q = rms(cq[...], gain(qg_ref)).astype(BF)
    cq[...] = c_q.astype(F4)

    def put(ref, h, val):
        for g in range(tokens // SUB):
            ref[g, h] = val[g * SUB:(g + 1) * SUB]

    def uq_step(i, carry):
        parts = []
        for k in range(2):
            b = B_Q + 2 * i + k
            slot = lax.rem(b, DEPTH_B)
            copy(uq.at[:, 0:Q_TILE], wB.at[slot, 0:q_rank, 0:Q_TILE], semB.at[slot]).wait()
        for k in range(2):
            b = B_Q + 2 * i + k
            parts.append(dot(cq[...].astype(BF), wB[lax.rem(b, DEPTH_B), 0:q_rank, 0:Q_TILE]).astype(BF).astype(F4))
        for k in range(2):
            issueB(B_Q + 2 * i + k + DEPTH_B)
        for h in range(4):
            q2 = parts[h // 2]
            base = (h % 2) * QK_DIM
            QN[4 * i + h] = q2[:, base:base + NOPE_DIM].astype(BF)
            put(QR, 4 * i + h, rotate(q2[:, base + NOPE_DIM:base + QK_DIM]).astype(BF).astype(F4))
        return carry

    lax.fori_loop(0, n_q // 2, uq_step, 0)

    cnew_ref[...] = rms(kvs[:, 0:rank], gain(kg_ref)).astype(BF)
    knew_ref[...] = rotate(kvs[:, rank:rank + ROPE_DIM]).astype(BF)
    c_out = copy(cnew_ref, cnew_hbm, semM.at[9])
    k_out = copy(knew_ref, knew_hbm, semM.at[10])
    c_out.start()
    k_out.start()

    waitB(B_UK)
    slot_uk = B_UK % DEPTH_B

    for h in range(HEADS):
        w_h = wB[slot_uk, (h // 4) * rank:(h // 4 + 1) * rank, (h % 4) * NOPE_DIM:(h % 4 + 1) * NOPE_DIM]
        put(QA, h, dot_t(QN[h], w_h).astype(BF).astype(F4))
    issueB(jnp.int32(B_UK + DEPTH_B))

    waitB(B_CKV)
    slot_ckv = B_CKV % DEPTH_B
    small[1].wait()
    span = SUB * CACHE
    scale = QK_DIM ** -0.5
    lane = lax.broadcasted_iota(jnp.int32, (SUB, span), 1)
    tok = lax.broadcasted_iota(jnp.int32, (SUB, span), 0)
    for g in range(tokens // SUB):
        keys = wB[slot_ckv, g * span:(g + 1) * span, :]
        qa = QA[g]
        qr = QR[g]
        cn = cnew_ref[g * SUB:(g + 1) * SUB, :].astype(F4)
        kn = knew_ref[g * SUB:(g + 1) * SUB, :].astype(F4)
        s = dot_t(qa.reshape(HEADS * SUB, rank).astype(BF), keys)
        s = s + dot_t(qr.reshape(HEADS * SUB, ROPE_DIM).astype(BF), kp[g * span:(g + 1) * span, :])
        s = s.reshape(HEADS, SUB, span) * scale
        limit = posv[g * SUB:(g + 1) * SUB, 0:1]
        valid = (lane >= tok * CACHE) & (lane < tok * CACHE + limit)
        s = jnp.where(valid[None], s, -1e30)
        s_self = (jnp.sum(qa * cn[None], axis=2, keepdims=True) + jnp.sum(qr * kn[None], axis=2, keepdims=True)) * scale
        peak = jnp.maximum(jnp.max(s, axis=2, keepdims=True), s_self)
        e = jnp.where(valid[None], jnp.exp(s - peak), 0.0)
        e_self = jnp.exp(s_self - peak)
        denom = jnp.sum(e, axis=2, keepdims=True) + e_self
        p = (e / denom).astype(BF)
        p_self = (e_self / denom).astype(BF).astype(F4)
        ctx = dot(p.reshape(HEADS * SUB, span), keys).reshape(HEADS, SUB, rank) + p_self * cn[None]
        QA[g] = ctx.astype(BF).astype(F4)
    issueB(jnp.int32(B_CKV + DEPTH_B))

    waitB(B_UV)
    slot_uv = B_UV % DEPTH_B
    for h in range(HEADS):
        w_h = wB[slot_uv, (h // 4) * rank:(h // 4 + 1) * rank, (h % 4) * VALUE_DIM:(h % 4 + 1) * VALUE_DIM]
        O[:, h * VALUE_DIM:(h + 1) * VALUE_DIM] = dot(QA[:, h].reshape(tokens, rank).astype(BF), w_h).astype(BF)
    issueB(jnp.int32(B_UV + DEPTH_B))

    pl.semaphore_wait(barrier, 7)

    def grp_x(p, block):
        return rcopy(xm.at[:, cols(p, GROUP)], U.at[rows(block), cols(p, GROUP)], px_s.at[p], px_r.at[p], X)

    def grp_y(p, block):
        return rcopy(xm.at[:, cols(p, GROUP)], U.at[rows(block), cols(p, GROUP)], py_s.at[p], py_r.at[p], Y)

    def pass_y(p, block):
        return rcopy(U.at[rows(kX), cols(p, GROUP)], U.at[rows(block), cols(p, GROUP)], pr_s.at[p], pr_r.at[p], Y)

    def pass_x(p, block):
        return rcopy(U.at[rows(kY), cols(p, GROUP)], U.at[rows(block), cols(p, GROUP)], pr_s.at[p], pr_r.at[p], X)

    def forward(p):
        odd = lax.rem(p, 2)

        @pl.when(odd == 0)
        def _():
            grp_x(p, kX).wait_recv()
            pass_y(p, kX).start()

        @pl.when(odd == 1)
        def _():
            grp_y(p, kY).wait_recv()
            pass_x(p, kY).start()

    def send_rest(first, last):
        for p in range(first, last):
            if p % 2 == 0:
                grp_y(p, chip).start()
            else:
                grp_x(p, chip).start()

    def out_step(i, carry):
        b = B_O + 2 * i
        waitB(b)
        waitB(b + 1)
        both = [dot(O[...], wB[lax.rem(b + k, DEPTH_B)]) for k in range(2)]
        for k in range(2):
            s = cols(2 * i + k, COL_TILE)
            xm[:, s] = (hid[:, s].astype(F4) + both[k]).astype(BF)
        grp_x(2 * i, chip).start()
        grp_y(2 * i + 1, chip).start()
        issueB(b + DEPTH_B)
        issueB(b + 1 + DEPTH_B)

        @pl.when(i < PASS_LAG)
        def _():
            grp_y(2 * i, chip).start()
            grp_x(2 * i + 1, chip).start()

        @pl.when(i >= PASS_LAG)
        def _():
            forward(2 * (i - PASS_LAG))
            forward(2 * (i - PASS_LAG) + 1)

        @pl.when((i >= A_AT) & (i < A_AT + DEPTH_A))
        def _():
            issueA(i - A_AT + n_dq)
        return carry

    lax.fori_loop(0, n_col // 2, out_step, 0)
    send_rest(2 * PASS_LAG, 2 * PASS_LAG + 2)

    small[8].wait()
    u_own = rms(xm[...].astype(F4), gain(fg_ref)).astype(BF)
    U[own, :] = u_own
    toS = rcopy(U.at[own, :], U.at[rows(4 + chip), :], d_s.at[0], d_r.at[0], sib)
    toS.start()
    small[2].wait()
    small[3].wait()
    experts = router.shape[0]
    capacity = (CAP_FACTOR * tokens * topk_ref.shape[0] + experts - 1) // experts
    gates = jax.nn.sigmoid(dot_t(U[own, :], wR[...]))
    eid = lax.broadcasted_iota(jnp.int32, (experts, tokens), 0)
    picks = jnp.zeros((experts, tokens), F4)
    for k in range(topk_ref.shape[0]):
        picks = picks + jnp.where(topk_ref[k:k + 1, :] == eid, 1.0, 0.0)
    picks = picks.astype(BF)
    here = lax.broadcasted_iota(jnp.int32, (tokens, tokens), 0)
    there = lax.broadcasted_iota(jnp.int32, (tokens, tokens), 1)
    hits = dot_t(jnp.where(here == there, 1.0, 0.0).astype(BF), picks)
    before = dot_t(jnp.where(here > there, 1.0, 0.0).astype(BF), picks)
    total = jnp.sum(hits * gates, axis=1, keepdims=True)
    table = jnp.where(before < capacity, hits, 0.0) * (ROUTE_SCALE * gates / total)
    WT[own, 0:experts] = table

    WT[own, experts:LANES] = jnp.zeros((tokens, LANES - experts), F4)
    D = kD * 2 + core
    mates = ((1, kX, X), (2, kY, Y), (3, kD, D))

    def table_to(i, dev):
        return rcopy(WT.at[own, :], WT.at[own, :], w_s.at[i], w_r.at[i], dev)

    def table_from(i, k, dev):
        return rcopy(WT.at[rows(k), :], WT.at[rows(k), :], w_s.at[i], w_r.at[i], dev)

    def tables_to_twin():
        return rcopy(WT.at[0:4 * tokens, :], WT.at[4 * tokens:8 * tokens, :], w_s.at[0], w_r.at[0], sib)

    for i, _, dev in mates:
        table_to(i, dev).start()

    def gated(both):
        g = both[:, 0:FF_TILE]
        return (g * jax.nn.sigmoid(g) * both[:, FF_TILE:2 * FF_TILE]).astype(BF)

    def to_twin(i, k):
        return rcopy(U.at[rows(k), :], U.at[rows(4 + k), :], d_s.at[i], d_r.at[i], sib)

    def normalise(block):
        r = rows(block)
        U[r, :] = rms(U[r, :].astype(F4), gain(fg_ref)).astype(BF)

    for p in range(n_grp - 2 * PASS_LAG, n_grp, 2):
        forward(jnp.int32(p))
        forward(jnp.int32(p + 1))
        if p > n_grp - 2 * PASS_LAG:
            q = p - n_grp + 4 * PASS_LAG
            send_rest(min(q, n_grp), min(q + 2, n_grp))
    send_rest(4 * PASS_LAG, n_grp)
    for p in range(1, n_grp, 2):
        grp_x(p, kX).wait_recv()
        pass_x(p, kY).wait_send()
    for p in range(0, n_grp, 2):
        pass_y(p, kX).wait_send()
    normalise(kX)
    to_twin(1, kX).start()
    for p in range(0, n_grp, 2):
        grp_y(p, kY).wait_recv()
    normalise(kY)
    to_twin(2, kY).start()
    for p in range(n_grp):
        if p % 2 == 0:
            pass_y(p, kD).wait_recv()
        else:
            pass_x(p, kD).wait_recv()
    normalise(kD)
    to_twin(3, kD).start()
    wait_pair(A_S0)
    part_s[0:4 * tokens, :] = gated(dot(U[0:4 * tokens, :], wA[A_S0 % DEPTH_A]))
    wait_pair(A_R)
    H[0, 0:4 * tokens, :] = dot(U[0:4 * tokens, :], wA[A_R % DEPTH_A])
    for i, k, dev in mates:
        table_from(i, k, dev).wait_recv()
    tables_to_twin().start()
    rcopy(U.at[own, :], U.at[rows(4 + chip), :], d_s.at[0], d_r.at[0], sib).wait_recv()
    for i, k in ((1, kX), (2, kY), (3, kD)):
        rcopy(U.at[rows(k), :], U.at[rows(4 + k), :], d_s.at[i], d_r.at[i], sib).wait_recv()
    part_s[4 * tokens:8 * tokens, :] = gated(dot(U[4 * tokens:8 * tokens, :], wA[A_S0 % DEPTH_A]))
    issueA(jnp.int32(A_S0 + DEPTH_A))
    H[0, 4 * tokens:8 * tokens, :] = dot(U[4 * tokens:8 * tokens, :], wA[A_R % DEPTH_A])
    issueA(jnp.int32(A_R + DEPTH_A))
    toS.wait_send()
    for i, k in ((1, kX), (2, kY), (3, kD)):
        to_twin(i, k).wait_send()
    for p in range(n_grp):
        grp_x(p, chip).wait_send()
        grp_y(p, chip).wait_send()

    def act_to(k):
        dev = lax.rem(me + k, 8)
        block = dev // 2 + 4 * lax.rem(core + dev, 2)
        return rcopy(part_s.at[rows(block), :], acts.at[:, cols(me, FF_TILE)], as_s.at[k], as_r.at[k], dev)

    def act_from(k):
        dev = lax.rem(me + 8 - k, 8)
        return rcopy(part_s.at[own, :], acts.at[:, cols(dev, FF_TILE)], as_s.at[k], as_r.at[k], dev)

    for k in range(1, 8):
        act_to(k).start()
    acts[:, cols(me, FF_TILE)] = part_s[own, :]

    def routed_up_step(i, carry):
        t = A_R + i
        wait_pair(t)
        last = i - 1
        ACT[last // n_ff, :, cols(lax.rem(last, n_ff), FF_TILE)] = gated(H[lax.rem(last, 2)])
        H[lax.rem(i, 2)] = dot(U[...], wA[lax.rem(t, DEPTH_A)])
        issueA(t + DEPTH_A)
        return carry

    lax.fori_loop(1, 2 * n_ff, routed_up_step, 0)
    ACT[1, :, ff - FF_TILE:ff] = gated(H[(2 * n_ff - 1) % 2])

    for i, _, dev in mates:
        table_to(i, dev).wait_send()
    tables_to_twin().wait()

    lane_id = lax.broadcasted_iota(jnp.int32, WT.shape, 1)
    w0 = jnp.sum(jnp.where(lane_id == 2 * me, WT[...], 0.0), axis=1, keepdims=True)
    w1 = jnp.sum(jnp.where(lane_id == 2 * me + 1, WT[...], 0.0), axis=1, keepdims=True)

    def to_sib(j):
        return rcopy(Ps.at[lax.rem(j, SIB_SLOTS)], R1.at[:, :, cols(j, COL_TILE)], sib_s.at[j], sib_r.at[j], sib)

    def first_leg(j, dev):
        return rcopy(Pm.at[kD, :, cols(j, COL_TILE)], RL.at[:, cols(j, COL_TILE)], rl_s.at[j], rl_r.at[j], dev)

    def last_x(j):
        return rcopy(Pm.at[kX, :, cols(j, COL_TILE)], RX.at[:, cols(j, COL_TILE)], x_s.at[j], x_r.at[j], X)

    def last_y(j):
        return rcopy(Pm.at[kY, :, cols(j, COL_TILE)], RY.at[:, cols(j, COL_TILE)], y_s.at[j], y_r.at[j], Y)

    def chip_sum(j):
        to_sib(j).wait_recv()
        Pm[:, :, cols(j, COL_TILE)] = Pm[:, :, cols(j, COL_TILE)] + R1[:, :, cols(j, COL_TILE)]
        odd = lax.rem(j, 2)

        @pl.when(odd == 0)
        def _():
            first_leg(j, X).start()

            @pl.when(j < RELAY_LAG)
            def _():
                last_x(j).start()

        @pl.when(odd == 1)
        def _():
            first_leg(j, Y).start()

            @pl.when(j < RELAY_LAG)
            def _():
                last_y(j).start()

    def relay(j):
        odd = lax.rem(j, 2)

        @pl.when(odd == 0)
        def _():
            first_leg(j, X).wait_recv()
            Pm[kY, :, cols(j, COL_TILE)] = Pm[kY, :, cols(j, COL_TILE)] + RL[:, cols(j, COL_TILE)]
            last_y(j).start()

        @pl.when(odd == 1)
        def _():
            first_leg(j, Y).wait_recv()
            Pm[kX, :, cols(j, COL_TILE)] = Pm[kX, :, cols(j, COL_TILE)] + RL[:, cols(j, COL_TILE)]
            last_x(j).start()

    def down_step(j, carry):
        b = B_D + 2 * j
        waitB(b)
        waitB(b + 1)
        e0 = dot(ACT[0], wB[lax.rem(b, DEPTH_B)]).astype(BF)
        e1 = dot(ACT[1], wB[lax.rem(b + 1, DEPTH_B)]).astype(BF)

        @pl.when(j >= SIB_SLOTS)
        def _():
            to_sib(j - SIB_SLOTS).wait_send()

        part = w0 * e0.astype(F4) + w1 * e1.astype(F4)
        Pm[:, :, cols(j, COL_TILE)] = part[0:4 * tokens].reshape(4, tokens, COL_TILE)
        Ps[lax.rem(j, SIB_SLOTS)] = part[4 * tokens:8 * tokens].reshape(4, tokens, COL_TILE)
        to_sib(j).start()
        issueB(b + DEPTH_B)
        issueB(b + 1 + DEPTH_B)

        @pl.when(j >= SIB_LAG)
        def _():
            chip_sum(j - SIB_LAG)

        @pl.when(j >= RELAY_LAG)
        def _():
            relay(j - RELAY_LAG)
        return carry

    lax.fori_loop(0, n_col, down_step, 0)
    for j in range(n_col - SIB_LAG, n_col):
        chip_sum(jnp.int32(j))
    for j in range(RELAY_LAG, n_col):
        if j % 2 == 0:
            last_x(jnp.int32(j)).start()
        else:
            last_y(jnp.int32(j)).start()
    relayed = n_col - RELAY_LAG

    for k in range(1, 8):
        act_from(k).wait_recv()
        act_to(k).wait_send()

    def result(j):
        return copy(out_ref.at[:, cols(j, COL_TILE)], out_hbm.at[:, cols(j, COL_TILE)], semM.at[11])

    def finish(j, carry):
        last_x(j).wait_recv()
        last_y(j).wait_recv()
        s = cols(j, COL_TILE)
        routed = Pm[chip, :, s] + RX[:, s] + RY[:, s]
        out_ref[:, s] = (xm[:, s].astype(F4) + routed + out_ref[:, s].astype(F4)).astype(BF)
        result(j).start()
        return carry

    def shared_down_step(j, carry):
        b = B_S + j
        waitB(b)
        out_ref[:, cols(j, COL_TILE)] = dot(acts[...], wB[lax.rem(b, DEPTH_B)]).astype(BF)
        issueB(b + DEPTH_B)

        @pl.when(relayed + j < n_col)
        def _():
            relay(relayed + j)

        @pl.when(j >= DONE_LAG)
        def _():
            finish(j - DONE_LAG, 0)
        return carry

    lax.fori_loop(0, n_col, shared_down_step, 0)
    lax.fori_loop(n_col - DONE_LAG, n_col, finish, 0)
    for j in range(n_col):
        if j >= n_col - SIB_SLOTS:
            to_sib(j).wait_send()
        first_leg(j, X).wait_send()
        last_x(j).wait_send()
        last_y(j).wait_send()
    c_out.wait()
    k_out.wait()
    copy(out_ref, out_hbm, semM.at[11]).wait()


def hand_on(a, b, c, oa, ob, oc, va, vb, vc, sems):
    pairs = ((a, va, oa), (b, vb, ob), (c, vc, oc))
    for i, (src, mid, _) in enumerate(pairs):
        pltpu.make_async_copy(src, mid, sems.at[0, i]).start()
    for i, (src, mid, dst) in enumerate(pairs):
        pltpu.make_async_copy(src, mid, sems.at[0, i]).wait()
        pltpu.make_async_copy(mid, dst, sems.at[1, i]).start()
    for i, (_, mid, dst) in enumerate(pairs):
        pltpu.make_async_copy(mid, dst, sems.at[1, i]).wait()


def layer_call(positions, topk_ids, gains, big):
    hidden, w_dq, w_uq = big[0], big[3], big[4]
    tokens, width = hidden.shape
    q_rank = w_dq.shape[1]
    rank = big[1].shape[1]
    ff = big[10].shape[1]
    total = 8 * tokens
    n_col = width // COL_TILE
    n_grp = width // GROUP
    half = ROPE_DIM // 2
    freq = np.zeros((8, LANES), np.float32)
    freq[0, :ROPE_DIM] = np.tile((ROPE_BASE ** (-np.arange(half) / half)).astype(np.float32), 2)
    freq[1, :ROPE_DIM] = np.repeat([-1.0, 1.0], half)
    smem = pl.BlockSpec(memory_space=pltpu.SMEM)
    hbm = pl.BlockSpec(memory_space=pl.ANY)
    dma = pltpu.SemaphoreType.DMA
    shapes = [(tokens, width), (tokens, rank), (tokens, ROPE_DIM)]
    outs = tuple(jax.ShapeDtypeStruct(shape, BF) for shape in shapes)
    results = pl.pallas_call(
        layer_kernel,
        out_shape=outs,
        in_specs=[smem] + [hbm] * (6 + len(big)),
        out_specs=(hbm, hbm, hbm),
        scratch_shapes=[pltpu.VMEM(topk_ids.shape, jnp.int32), pltpu.VMEM(freq.shape, F4)]
        + [pltpu.VMEM(g.shape, BF) for g in gains] + [pltpu.VMEM(shape, BF) for shape in shapes] + [
            pltpu.VMEM((total, width), BF),
            pltpu.VMEM((total, LANES), F4),
            pltpu.VMEM((DEPTH_A, width, 2 * FF_TILE), BF),
            pltpu.VMEM((DEPTH_B, ff, COL_TILE), BF),
            pltpu.VMEM(big[9].shape, BF),
            pltpu.VMEM(big[2].shape, BF),
            pltpu.VMEM((tokens, big[5].shape[0]), F4),
            pltpu.VMEM((tokens, width), BF),
            pltpu.VMEM((tokens, width), BF),
            pltpu.VMEM((tokens, q_rank), F4),
            pltpu.VMEM((HEADS, tokens, NOPE_DIM), BF),
            pltpu.VMEM((tokens // SUB, HEADS, SUB, rank), F4),
            pltpu.VMEM((tokens // SUB, HEADS, SUB, ROPE_DIM), F4),
            pltpu.VMEM((tokens, HEADS * VALUE_DIM), BF),
            pltpu.VMEM((tokens, ff), BF),
            pltpu.VMEM((total, FF_TILE), BF),
            pltpu.VMEM((2, total, 2 * FF_TILE), F4),
            pltpu.VMEM((2, total, ff), BF),
            pltpu.VMEM((4, tokens, width), F4),
            pltpu.VMEM((SIB_SLOTS, 4, tokens, COL_TILE), F4),
            pltpu.VMEM((4, tokens, width), F4),
            pltpu.VMEM((tokens, width), F4),
            pltpu.VMEM((tokens, width), F4),
            pltpu.VMEM((tokens, width), F4),
            dma((2, DEPTH_A)), dma((DEPTH_B,)), dma((12,)), dma((8,)), dma((8,)),
        ] + [dma((n_grp,))] * 6 + [dma((4,))] * 4 + [dma((n_col,))] * 8,
        compiler_params=pltpu.CompilerParams(collective_id=0, has_side_effects=True, vmem_limit_bytes=67043328),
        name='decode_layer',
    )(positions, topk_ids, jnp.asarray(freq), *gains, *big)
    return pl.pallas_call(
        hand_on,
        out_shape=outs,
        in_specs=[hbm] * 3,
        out_specs=(hbm, hbm, hbm),
        scratch_shapes=[pltpu.VMEM(shape, BF) for shape in shapes] + [dma((2, 3))],
        name='hand_on',
    )(*results)


def solution(mesh):
    batch = P(('dp', 'ep'))
    whole = P()
    by_expert = P('ep')

    def local_step(hidden, positions, ckv_cache, kpe_cache, topk_ids, attn_gain, w_dq, q_gain, w_uq, w_dkv, kv_gain, w_uk, w_uv, w_out, ffn_gain, w_router, w_gate, w_up, w_down, shared_gate, shared_up, shared_down):
        gains = [attn_gain, q_gain, kv_gain, ffn_gain]
        ckv = ckv_cache.reshape(-1, ckv_cache.shape[2])
        kpe = kpe_cache.reshape(-1, kpe_cache.shape[2])
        big = (hidden, ckv, kpe, w_dq, w_uq, w_dkv.T, w_uk, w_uv, w_out, w_router.T, shared_gate, shared_up, shared_down, w_gate, w_up, w_down)
        return layer_call(positions, topk_ids.T, gains, big)

    in_specs = (batch,) * 5 + (whole,) * 11 + (by_expert,) * 3 + (whole,) * 3
    return jax.shard_map(local_step, mesh=mesh, in_specs=in_specs, out_specs=(batch, batch, batch), check_vma=False)
```
